32 devices in a mesh: dp: 2 (over core), seq: 4 (over z), tensor: 4 (over y, x).
Axes of the slice: x: 2, y: 2, z: 4, core: 2. Of those that a mesh axis runs over, the one named last changes fastest.
Arguments:
- tokens: bfloat16 [256, 4, 5120], P('seq', 'dp'), parts along dimension 1, may hold values from -6 to 6
- w_query: bfloat16 [5120, 5120], P(None, 'tensor'), may hold values from -0.5 to 0.5, as said below
- w_key: bfloat16 [5120, 5120], P(None, 'tensor'), may hold values from -0.5 to 0.5, as said below
- w_value: bfloat16 [5120, 5120], P(None, 'tensor'), may hold values from -0.078125 to 0.078125
- w_out: bfloat16 [5120, 5120], P('tensor'), may hold values from -0.125 to 0.125
- gain_query: float32 [5120], P('tensor'), may hold values from 0.5 to 4
- gain_key: float32 [5120], P('tensor'), may hold values from 0.5 to 4
Outputs:
- attended: bfloat16 [256, 4, 5120], P(('seq', 'tensor'), 'dp'), parts along dimension 1
The draws below stay inside these ranges and needn't reach their ends.
There are 2 independent parts, one for each index of `dp`. The reference program is written for one: setup_inputs(seed, part) draws one part's arguments, and reference() takes and returns one part's arrays. A program takes and returns all parts, laid end to end along the dimension named above; an argument that names none is the same for every part. Nothing has to cross between parts.
Inputs may be any that keep to these rules, and one draw needn't show every extreme that they name: `w_query`: entries of order 5120 ** -0.5 with unequal column scales. `w_key`: entries of order 5120 ** -0.5 with unequal column scales.
All inputs are finite; a program needn't handle non-finite values.
Results may differ from the reference program's by a relative error of at most 0.013.
The reference program's roundings to bfloat16 on the way count: a program that leaves them out, or rounds other values in their place, can miss the bound.
Values may be sent and summed in bfloat16 or wider, within the bound.
A program may use at most 256 MiB of HBM per device.

```python
import jax
import jax.numpy as jnp
from jax import lax

D = 5120
HEADS = 40
HEAD_DIM = 128
SEQS = 2
TOK_DEV = 64
SEQ = 256


def ramped_weight(key, salt):
    width = HEADS * HEAD_DIM
    first, second = jax.random.split(jax.random.fold_in(key, salt))
    base = jax.random.truncated_normal(first, -4.0, 4.0, (D, width), jnp.float32)
    heads = (jnp.arange(width) // HEAD_DIM).astype(jnp.float32)
    ramp = jnp.exp(jnp.log(0.6) + jnp.log(3.0) * heads / max(HEADS - 1, 1))
    upper = 3.3
    column = jnp.exp(jax.random.uniform(second, (width,), jnp.float32) * jnp.log(upper))
    scaled = base * (ramp * column)[None, :] / jnp.sqrt(jnp.float32(D))
    return jnp.clip(scaled, -0.5, 0.5).astype(jnp.bfloat16)


def drawn_gain(key, salt):
    width = HEADS * HEAD_DIM
    lower, upper = (0.5, 2.0)
    sample = jax.random.uniform(jax.random.fold_in(key, salt), (width,), jnp.float32, jnp.log(lower), jnp.log(upper))
    return jnp.exp(sample).astype(jnp.float32)


def draw_w_query(key, part):
    return ramped_weight(key, 11)


def draw_w_key(key, part):
    return ramped_weight(key, 23)


def draw_gain_query(key, part):
    return drawn_gain(key, 37)


def draw_gain_key(key, part):
    return drawn_gain(key, 41)


def with_spikes(entries, rng, source, target, parts, factor):
    def block_of(axis_at):
        return (jnp.arange(entries.shape[axis_at]) // (entries.shape[axis_at] // parts)).reshape((-1,) + (1,) * (entries.ndim - 1 - axis_at))

    one_side = jax.random.permutation(rng, parts)[block_of(target)]
    other_side = (block_of(target) + parts // 2) % parts
    return jnp.where((block_of(source) == one_side) | (block_of(source) == other_side), factor * entries, entries)


def steps_of(key, dims, shards, smallest, largest):
    level = 1.0
    for axis_at, parts in shards:
        heights = jax.random.uniform(jax.random.fold_in(jax.random.fold_in(key, 6), axis_at), (parts,), jnp.float32, smallest / len(shards), largest / len(shards))
        level = level * jnp.repeat(jnp.exp(heights), dims[axis_at] // parts).reshape((-1,) + (1,) * (len(dims) - 1 - axis_at))
    return level


def bell_draw(key, dims, spread, reach, cuts=(), held_as=jnp.bfloat16):
    loudness = steps_of(key, dims, cuts, -0.22, 0.18) if cuts else 1.0
    entries = jax.random.normal(key, dims, jnp.float32) * spread * loudness
    return jnp.minimum(jnp.maximum(entries, -reach), reach).astype(held_as)


def bell_draw_with(key, dims, scale, reach, cuts, heavy, kind=jnp.bfloat16):
    drawn = scale * jax.random.normal(key, dims, jnp.float32)
    if cuts:
        drawn = drawn * steps_of(key, dims, cuts, -0.22, 0.18)
    return jnp.clip(with_spikes(drawn, jax.random.fold_in(key, 3), *heavy), -reach, reach).astype(kind)


def setup_inputs(seed: int = 0, part: int = 0) -> dict:
    seeds = jax.random.split(jax.random.key(seed), 8)
    part_splits = jax.random.split(jax.random.fold_in(seeds[7], part), 8)
    return {
        "tokens": bell_draw(part_splits[0], (SEQ, SEQS, D), 1.0, 6.0, ((0, 4),)),
        "w_query": draw_w_query(jax.random.fold_in(seeds[7], 71), part),
        "w_key": draw_w_key(jax.random.fold_in(seeds[7], 71), part),
        "w_value": bell_draw(seeds[3], (D, HEADS * HEAD_DIM), D ** -0.5, 0.078125, ((1, 4),)),
        "w_out": bell_draw_with(seeds[4], (HEADS * HEAD_DIM, D), (HEADS * HEAD_DIM) ** -0.5, 0.125, ((0, 4),), (0, 1, 4, 2.0)),
        "gain_query": draw_gain_query(jax.random.fold_in(seeds[7], 71), part),
        "gain_key": draw_gain_key(jax.random.fold_in(seeds[7], 71), part),
    }


def rotary(field, positions):
    half = HEAD_DIM // 2
    shaped = field.reshape(field.shape[0], -1, HEAD_DIM)
    freqs = jnp.exp(-jnp.log(500000.0) * jnp.arange(half, dtype=jnp.float32) * 2.0 / HEAD_DIM)
    angle = positions.astype(jnp.float32)[:, None] * freqs[None, :]
    cosine = jnp.cos(angle)[:, None, :]
    sine = jnp.sin(angle)[:, None, :]
    first = shaped[..., :half]
    second = shaped[..., half:]
    turned = jnp.concatenate([first * cosine - second * sine, second * cosine + first * sine], axis=-1)
    return turned.reshape(field.shape[0], -1)

def one_sequence(seq_tokens, w_query, w_key, w_value, w_out, gain_query, gain_key):
    width = HEADS * HEAD_DIM
    query = jnp.dot(seq_tokens, w_query, preferred_element_type=jnp.float32)
    key_raw = jnp.dot(seq_tokens, w_key, preferred_element_type=jnp.float32)
    value = jnp.dot(seq_tokens, w_value, preferred_element_type=jnp.float32).astype(jnp.bfloat16)
    scale_q = lax.rsqrt(lax.optimization_barrier(jnp.sum(query * query, axis=1)) / width + 1e-06)
    scale_k = lax.rsqrt(lax.optimization_barrier(jnp.sum(key_raw * key_raw, axis=1)) / width + 1e-06)
    positions = jnp.arange(SEQ, dtype=jnp.int32)
    q_normed = rotary(query * scale_q[:, None] * gain_query[None, :], positions).astype(jnp.bfloat16)
    k_normed = rotary(key_raw * scale_k[:, None] * gain_key[None, :], positions).astype(jnp.bfloat16)
    keys_all = k_normed.reshape(SEQ, HEADS, HEAD_DIM).astype(jnp.float32)
    values_all = value.reshape(SEQ, HEADS, HEAD_DIM).astype(jnp.float32)
    factor = HEAD_DIM ** (-0.5)

    def one_block(index):
        start = (index * TOK_DEV).astype(jnp.int32)
        q_block = lax.dynamic_slice_in_dim(q_normed, start, TOK_DEV, 0).reshape(TOK_DEV, HEADS, HEAD_DIM).astype(jnp.float32)
        scores = jnp.einsum('qhd,khd->hqk', q_block, keys_all) * factor
        q_pos = start + jnp.arange(TOK_DEV, dtype=jnp.int32)
        allowed = positions[None, None, :] <= q_pos[None, :, None]
        top = lax.optimization_barrier(jnp.max(jnp.where(allowed, scores, -1e+30), axis=2))
        expo = jnp.where(allowed, jnp.exp(scores - top[..., None]), 0.0)
        total = lax.optimization_barrier(jnp.sum(expo, axis=2))
        rounded = expo.astype(jnp.bfloat16).astype(jnp.float32)
        summed = jnp.einsum('hqk,khd->hqd', rounded, values_all)
        mixed = (summed / total[..., None]).astype(jnp.bfloat16)
        return jnp.transpose(mixed, (1, 0, 2)).reshape(TOK_DEV, width)
    blocks = lax.map(one_block, jnp.arange(SEQ // TOK_DEV, dtype=jnp.int32))
    mixed_all = blocks.reshape(SEQ, width)
    return jnp.dot(mixed_all, w_out, preferred_element_type=jnp.float32).astype(jnp.bfloat16)

def reference(tokens, w_query, w_key, w_value, w_out, gain_query, gain_key):
    by_sequence = jnp.transpose(tokens, (1, 0, 2))

    def handle(seq_tokens):
        return one_sequence(seq_tokens, w_query, w_key, w_value, w_out, gain_query, gain_key)
    results = lax.map(handle, by_sequence)
    return jnp.transpose(results, (1, 0, 2))
```

```python
import contextlib
import functools

import jax
import jax.numpy as jnp
from jax import lax
from jax.experimental import pallas as pl
from jax.experimental.pallas import tpu as pltpu
from jax.sharding import PartitionSpec as P

HEADS = 40
HEAD_DIM = 128
MESH = pl.DeviceIdType.MESH
COLS = 2 * HEAD_DIM
RING = 9
F32 = jnp.float32
BF16 = jnp.bfloat16


def scope(name):
    return contextlib.nullcontext()


def block_kernel(
    ns, nt, tok, width,
    x_hbm, gq_in, gk_in, wq, wk, wv, wo,
    out_ref,
    ring, wov, xin, xi, xs, cos_ref, sin_ref, gains, ssq,
    sums_out, sums_in, sums_far, rqs, rks,
    qk, vbuf, own_o, own_lse, oout, lse_out, lse_msg, oin, lse_in, shares,
    mixed, part, rs_in,
    x_sem, w_sem, wo_sem, sum_send, sum_recv, far_send, far_recv, k_send, k_recv, v_send, v_recv,
    q_send, q_recv, o_send, o_recv, l_send, l_recv, rs_send, rs_recv,
):
    dp = lax.axis_index("dp")
    z = lax.axis_index("seq")
    me = lax.axis_index("tensor")
    low = z < 2
    high = z >= 2
    nc = vbuf.shape[0]
    rows = 2 * tok
    oc = wov.shape[2]
    no = wov.shape[0]

    def w_copy(ref, c, slot):
        return pltpu.make_async_copy(
            ref.at[:, pl.ds(pl.multiple_of(c * COLS, COLS), COLS)], ring.at[slot], w_sem.at[slot]
        )

    def wo_copy(c):
        return pltpu.make_async_copy(
            wo.at[:, pl.ds(pl.multiple_of(c * oc, oc), oc)], wov.at[c], wo_sem.at[c]
        )

    def start(i):
        slot = lax.rem(i, RING)
        group = i // nc
        c = i - group * nc
        inside = i < 3 * nc

        @pl.when(inside & ((low & (group == 0)) | (high & (group == 1))))
        def _():
            w_copy(wk, c, slot).start()

        @pl.when(inside & (((z == 0) & (group == 1)) | ((z > 0) & (group == 2))))
        def _():
            w_copy(wv, c, slot).start()

        @pl.when(inside & (((z == 0) & (group == 2)) | ((z == 1) & (group == 1)) | (high & (group == 0))))
        def _():
            w_copy(wq, c, slot).start()

        @pl.when((i >= 3 * nc) & (i < 3 * nc + no))
        def _():
            wo_copy(i - 3 * nc).start()

    x_copy = pltpu.make_async_copy(x_hbm, xin, x_sem)
    x_copy.start()

    @pl.loop(0, RING - 1)
    def _(i):
        start(i)

    barrier = pltpu.get_barrier_semaphore()
    linked = {0: (1,), 1: (0, 2, 3), 2: (1, 3), 3: (1, 2)}
    for d in range(1, nt):
        pl.semaphore_signal(barrier, inc=1, device_id=(dp, z, lax.rem(me + d, nt)), device_id_type=MESH)
    for a in range(ns):
        hit = functools.reduce(jnp.logical_or, [z == b for b in linked[a]])

        @pl.when(hit)
        def _():
            for d in range(nt):
                pl.semaphore_signal(barrier, inc=1, device_id=(dp, a, lax.rem(me + d, nt)), device_id_type=MESH)

    def greet():
        pl.semaphore_wait(barrier, nt - 1 + nt * jnp.where(z == 0, 1, jnp.where(z == 1, 3, 2)))

    def remote(src, dst, ssem, rsem, to):
        return pltpu.make_async_remote_copy(
            src_ref=src, dst_ref=dst, send_sem=ssem, recv_sem=rsem, device_id=to, device_id_type=MESH
        )

    def k_copy(c, j, to):
        return remote(qk.at[0, c, j, pl.ds(0, tok)], qk.at[0, c, j, pl.ds(tok, tok)], k_send.at[j, c], k_recv.at[j, c], (dp, to, me))

    def v_copy(c, j, to):
        return remote(vbuf.at[c, j, pl.ds(0, tok)], vbuf.at[c, j, pl.ds(tok, tok)], v_send.at[j, c], v_recv.at[j, c], (dp, to, me))

    def q_copy(c, j, s, to):
        return remote(qk.at[1, c, j, pl.ds(0, tok)], qk.at[1, c, j, pl.ds(s * tok, tok)], q_send.at[s - 1, j, c], q_recv.at[s - 1, j, c], (dp, to, me))

    def o_copy(c, j, s, to):
        return remote(oout.at[s - 1, c, j], oin.at[s - 1, c, j], o_send.at[s - 1, j, c], o_recv.at[s - 1, j, c], (dp, to, me))

    def l_copy(j, s, to):
        return remote(lse_msg.at[j], lse_in.at[s - 1, j], l_send.at[s - 1, j], l_recv.at[s - 1, j], (dp, to, me))

    def near(g, d):
        return remote(sums_out.at[g], sums_in.at[g, d - 1], sum_send.at[g, d - 1], sum_recv.at[g, d - 1], (dp, z, lax.rem(me + d, nt)))

    def far(d, slot, ss, to):
        return remote(sums_out.at[0], sums_far.at[slot, d], far_send.at[ss, d], far_recv.at[slot, d], (dp, to, lax.rem(me + d, nt)))

    def product(i):
        slot = lax.rem(i, RING)
        start(i + RING - 1)
        with scope("wwait"):
            w_copy(wk, 0, slot).wait()
        return jnp.dot(xs[...], ring[slot], preferred_element_type=F32)

    def turned(acc, kind, c):
        cosine, sine = cos_ref[...], sin_ref[...]
        for h in range(2):
            y = acc[:, h * HEAD_DIM : (h + 1) * HEAD_DIM] * gains[kind, c, :, h * HEAD_DIM : (h + 1) * HEAD_DIM]
            y = (y * cosine + pltpu.roll(y, HEAD_DIM // 2, 1) * sine).astype(BF16)
            for j in range(2):
                qk[kind, c, j, 0:tok, h * HEAD_DIM : (h + 1) * HEAD_DIM] = y[j * tok : (j + 1) * tok]

    def finish(acc, kind, c):
        ssq[kind] += acc[:, :HEAD_DIM] * acc[:, :HEAD_DIM] + acc[:, HEAD_DIM:] * acc[:, HEAD_DIM:]
        turned(acc, kind, c)

    def keep_value(acc, c):
        v = acc.astype(BF16)
        for j in range(2):
            vbuf[c, j, 0:tok, :] = v[j * tok : (j + 1) * tok]

    with scope("init"):
        lanes = lax.broadcasted_iota(jnp.int32, (tok, HEAD_DIM), 1)
        half = HEAD_DIM // 2
        freqs = jnp.exp(-jnp.log(500000.0) * lax.rem(lanes, half).astype(F32) * 2.0 / HEAD_DIM)
        spot = z * tok + lax.broadcasted_iota(jnp.int32, (tok, HEAD_DIM), 0)
        angle = spot.astype(F32) * freqs
        cosine = jnp.cos(angle)
        sine = jnp.sin(angle)
        sine = jnp.where(lanes < half, -sine, sine)
        for j in range(2):
            cos_ref[j * tok : (j + 1) * tok] = cosine
            sin_ref[j * tok : (j + 1) * tok] = sine
        for c in range(nc):
            gains[0, c] = gk_in[c * COLS : (c + 1) * COLS].reshape(1, COLS)
            gains[1, c] = gq_in[c * COLS : (c + 1) * COLS].reshape(1, COLS)
        ssq[...] = jnp.zeros_like(ssq)
        sums_out[...] = jnp.zeros_like(sums_out)
        own_lse[...] = jnp.zeros_like(own_lse)
        lse_out[...] = jnp.zeros_like(lse_out)

    with scope("xwait"):
        x_copy.wait()
    with scope("xlay"):
        @pl.loop(0, tok // 8)
        def _(i):
            v = xin[pl.ds(pl.multiple_of(i * 8, 8), 8)]
            xi[pl.ds(pl.multiple_of(i * 16, 16), 16), :] = v.reshape(16, v.shape[-1])

        r = lax.broadcasted_iota(jnp.int32, (rows, rows), 0)
        q = lax.broadcasted_iota(jnp.int32, (rows, rows), 1)
        pick = (q == jnp.where(r < tok, 2 * r, 2 * (r - tok) + 1)).astype(F32).astype(BF16)

        half_depth = xs.shape[1] // 2
        for i in range(2):
            at = slice(i * half_depth, (i + 1) * half_depth)
            xs[:, at] = jnp.dot(pick, xi[:, at], preferred_element_type=F32).astype(BF16)

    def send_sums(g, kind):
        sums_out[g, 0:1, :] = jnp.sum(jnp.transpose(ssq[kind]), axis=0, keepdims=True)
        for d in range(1, nt):
            near(g, d).start()

    first = jnp.where(low, 0, 1)
    second = jnp.where(z == 1, 1, 0)

    with scope("g0"):
        @pl.loop(0, nc)
        def _(c):
            acc = product(c)

            @pl.when((c == 0) & (z != 1))
            def _():
                greet()

            finish(acc, first, c)

            @pl.when(z == 0)
            def _():
                k_copy(c, 0, 1).start()

            @pl.when(z == 3)
            def _():
                q_copy(c, 0, 2, 1).start()

    @pl.when(z == 1)
    def _():
        with scope("barwait"):
            greet()

    send_sums(0, first)

    @pl.when(z == 0)
    def _():
        for d in range(nt):
            far(d, 0, 0, 1).start()

    @pl.when(z == 2)
    def _():
        for d in range(nt):
            far(d, 1, 0, 1).start()

    @pl.when(z == 3)
    def _():
        for d in range(nt):
            far(d, 2, 0, 1).start()
        for d in range(nt):
            far(d, 2, 1, 2).start()

    with scope("g1"):
        @pl.loop(0, nc)
        def _(c):
            acc = product(nc + c)

            @pl.when(z == 0)
            def _():
                keep_value(acc, c)
                v_copy(c, 0, 1).start()

            @pl.when(z > 0)
            def _():
                finish(acc, second, c)

            @pl.when(z == 2)
            def _():
                q_copy(c, 0, 1, 1).start()

            @pl.when(z == 3)
            def _():
                q_copy(c, 0, 1, 2).start()

    @pl.when(z > 0)
    def _():
        send_sums(1, second)

    def near_scale(g):
        tot = sums_out[g]
        for d in range(1, nt):
            near(g, d).wait_recv()
            tot = tot + sums_in[g, d - 1]
        return lax.rsqrt(tot / width + 1e-06)

    def far_scale(slot):
        tot = None
        for d in range(nt):
            far(d, slot, 0, z).wait_recv()
            tot = sums_far[slot, d] if d == 0 else tot + sums_far[slot, d]
        return lax.rsqrt(tot / width + 1e-06)

    def set_rq(s, r):
        rqs[s] = jnp.transpose(jnp.broadcast_to(r[0:1, :] * HEAD_DIM ** (-0.5), (rows, rows)))

    def set_rk(r0, r1):
        left = lax.broadcasted_iota(jnp.int32, r0.shape, 1) < tok
        rks[0] = jnp.where(left, r0, pltpu.roll(r1, tok, 1))
        rks[1] = jnp.where(left, pltpu.roll(r0, tok, 1), r1)

    lane = lax.broadcasted_iota(jnp.int32, (tok, HEAD_DIM), 1)

    def attend(c, js, lo, hi, nk, merged):
        row = lax.broadcasted_iota(jnp.int32, (tok, nk * tok), 0)
        col = lax.broadcasted_iota(jnp.int32, (tok, nk * tok), 1)
        allowed = (col <= row) | (col >= tok)
        units = [(j, h, slice(h * HEAD_DIM, (h + 1) * HEAD_DIM)) for j in js for h in range(2)]
        spans = range(lo, hi)
        scores = [
            lax.dot_general(
                qk[1, c, j, lo * tok : hi * tok, hs], qk[0, c, j, 0 : nk * tok, hs],
                (((1,), (1,)), ((), ())), preferred_element_type=F32,
            )
            for j, h, hs in units
        ]
        scaled = []
        for (j, h, hs), score in zip(units, scores):
            for s in spans:
                sc = score[(s - lo) * tok : (s - lo + 1) * tok]
                sc = sc * rqs[s, j * tok : (j + 1) * tok, 0 : nk * tok] * rks[j, 0:1, 0 : nk * tok]
                scaled.append(jnp.where(allowed, sc, -1e30) if s == 0 else sc)
        tops = [jnp.max(sc, axis=1, keepdims=True) for sc in scaled]
        expos = [jnp.exp(sc - top) for sc, top in zip(scaled, tops)]
        tots = [jnp.sum(e, axis=1, keepdims=True) for e in expos]
        n = hi - lo
        accs = []
        for i, (j, h, hs) in enumerate(units):
            w = [e.astype(BF16) for e in expos[i * n : (i + 1) * n]]
            w = w[0] if n == 1 else jnp.concatenate(w, axis=0)
            accs.append(jnp.dot(w, vbuf[c, j, 0 : nk * tok, hs], preferred_element_type=F32))
        for i, (j, h, hs) in enumerate(units):
            for s in spans:
                o = accs[i][(s - lo) * tok : (s - lo + 1) * tok] / tots[i * n + s - lo]
                if s == 0 and not merged:
                    mixed[j * tok : (j + 1) * tok, pl.ds(pl.multiple_of(c * COLS + h * HEAD_DIM, HEAD_DIM), HEAD_DIM)] = o.astype(BF16)
                elif s == 0:
                    own_o[c, j, :, hs] = o
                else:
                    oout[s - 1, c, j, :, hs] = o.astype(BF16)
        if not merged:
            return
        for i, j in enumerate(js):
            for s in spans:
                a, b = (tops[u] + jnp.log(tots[u]) for u in (2 * i * n + s - lo, (2 * i + 1) * n + s - lo))
                if s > 0:
                    lse_out[j, s - 1] = jnp.where(lane == 2 * c, a, jnp.where(lane == 2 * c + 1, b, lse_out[j, s - 1]))
                else:
                    own_lse[j] = jnp.where(lane == 2 * c, a, jnp.where(lane == 2 * c + 1, b, own_lse[j]))

    def remote_part(c, j):
        @pl.when(z == 1)
        def _():
            with scope("attwait"):
                q_copy(c, j, 1, z).wait_recv()
                q_copy(c, j, 2, z).wait_recv()
                if j == 0:
                    k_copy(c, 0, z).wait_recv()
                    v_copy(c, 0, z).wait_recv()
            attend(c, (j,), 1, 3, 2, True)
            o_copy(c, j, 1, 2).start()
            o_copy(c, j, 2, 3).start()

        @pl.when(z == 2)
        def _():
            with scope("attwait"):
                q_copy(c, j, 1, z).wait_recv()
            attend(c, (j,), 0, 2, 1, True)
            o_copy(c, j, 1, 3).start()

    def send_lse(j):
        def message(a, b):
            lse_msg[j] = jnp.transpose(jnp.concatenate([a, b], axis=0))[0:16]

        @pl.when(z == 1)
        def _():
            message(lse_out[j, 0], lse_out[j, 1])
            l_copy(j, 1, 2).start()
            l_copy(j, 2, 3).start()

        @pl.when(z == 2)
        def _():
            message(lse_out[j, 0], lse_out[j, 0])
            l_copy(j, 1, 3).start()

    with scope("g2"):
        @pl.loop(0, nc)
        def _(c):
            acc = product(2 * nc + c)

            @pl.when(z == 0)
            def _():
                finish(acc, 1, c)
                k_copy(c, 1, 1).start()
                v_copy(c, 1, 1).start()

            @pl.when(z > 0)
            def _():
                keep_value(acc, c)

            @pl.when(z == 2)
            def _():
                q_copy(c, 1, 1, 1).start()

            @pl.when(z == 3)
            def _():
                q_copy(c, 1, 2, 1).start()
                q_copy(c, 1, 1, 2).start()

            @pl.when((c == 0) & (z == 1))
            def _():
                with scope("sumwait"):
                    set_rk(near_scale(0), far_scale(0))
                    set_rq(0, near_scale(1))
                    set_rq(1, far_scale(1))
                    set_rq(2, far_scale(2))

            @pl.when((c == 0) & high)
            def _():
                with scope("sumwait"):
                    set_rq(0, near_scale(0))
                    r = near_scale(1)
                    set_rk(r, r)

            @pl.when((c == 0) & (z == 2))
            def _():
                with scope("sumwait"):
                    set_rq(1, far_scale(2))

            remote_part(c, 0)

            @pl.when(z == 3)
            def _():
                attend(c, (0, 1), 0, 1, 1, True)

    send_lse(0)

    @pl.when(z == 0)
    def _():
        with scope("own"):
            send_sums(1, 1)
            r = near_scale(0)
            set_rk(r, r)
            set_rq(0, near_scale(1))

            @pl.loop(0, nc)
            def _(c):
                attend(c, (0, 1), 0, 1, 1, False)

    @pl.when(z == 1)
    def _():
        with scope("own"):
            @pl.loop(0, nc)
            def _(c):
                k_copy(c, 1, z).wait_recv()
                v_copy(c, 1, z).wait_recv()
                attend(c, (0, 1), 0, 1, 2, False)

    with scope("rem1"):
        @pl.when((z == 1) | (z == 2))
        def _():
            @pl.loop(0, nc)
            def _(c):
                remote_part(c, 1)

        send_lse(1)

    def merge(j, ni):
        lses = [own_lse[j]]
        for s in range(1, ni + 1):
            l_copy(j, s, z).wait_recv()
            wide = jnp.concatenate([lse_in[s - 1, j], jnp.zeros((rows - 16, rows), F32)], axis=0)
            lses.append(jnp.transpose(wide)[(ni - 1) * tok : ni * tok])
        top = functools.reduce(jnp.maximum, lses)
        parts = [jnp.exp(v - top) for v in lses]
        tot = functools.reduce(jnp.add, parts)
        for s in range(ni + 1):
            shares[s] = parts[s] / tot

        @pl.loop(0, nc)
        def _(c):
            for s in range(1, ni + 1):
                o_copy(c, j, s, z).wait_recv()
            for h in range(2):
                hs = slice(h * HEAD_DIM, (h + 1) * HEAD_DIM)
                o = 0.0
                for s in range(ni + 1):
                    share = jnp.sum(jnp.where(lane == 2 * c + h, shares[s], 0.0), axis=1, keepdims=True)
                    o += share * (own_o[c, j, :, hs] if s == 0 else oin[s - 1, c, j, :, hs].astype(F32))
                mixed[j * tok : (j + 1) * tok, pl.ds(pl.multiple_of(c * COLS + h * HEAD_DIM, HEAD_DIM), HEAD_DIM)] = o.astype(BF16)

    share = tok // nt

    def rs_copy(n, j, d):
        to = lax.rem(me + d, nt)
        return remote(
            part.at[n, j, pl.ds(pl.multiple_of(to * share, share), share)], rs_in.at[d - 1, n, j],
            rs_send.at[d - 1, j, n], rs_recv.at[d - 1, j, n], (dp, z, to),
        )

    for j in range(2):
        with scope("merge"):
            @pl.when(z == 2)
            def _():
                merge(j, 1)

            @pl.when(z == 3)
            def _():
                merge(j, 2)

        with scope("outp"):
            @pl.loop(0, no)
            def _(n):
                if j == 0:
                    wo_copy(n).wait()
                acc = jnp.dot(mixed[j * tok : (j + 1) * tok], wov[n], preferred_element_type=F32)
                part[n, j] = acc.astype(BF16)
                for d in range(1, nt):
                    rs_copy(n, j, d).start()

    with scope("rs"):
        for j in range(2):

            @pl.loop(0, no)
            def _(n):
                for d in range(1, nt):
                    rs_copy(n, j, d).wait_recv()
                o = part[n, j, pl.ds(pl.multiple_of(me * share, share), share)].astype(F32)
                for d in range(1, nt):
                    o += rs_in[d - 1, n, j].astype(F32)
                out_ref[:, j, pl.ds(pl.multiple_of(n * oc, oc), oc)] = o.astype(BF16)

    for j in range(2):

        @pl.loop(0, no)
        def _(n):
            for d in range(1, nt):
                rs_copy(n, j, d).wait_send()

    _t = scope("tail")
    _t.__enter__()
    for g in range(2):
        for d in range(1, nt):
            near(g, d).wait_send()

    @pl.when(z == 0)
    def _():
        for d in range(nt):
            far(d, 0, 0, 1).wait_send()

        @pl.loop(0, nc)
        def _(c):
            for j in range(2):
                k_copy(c, j, 1).wait_send()
                v_copy(c, j, 1).wait_send()

    @pl.when(z == 1)
    def _():
        for j in range(2):
            l_copy(j, 1, 2).wait_send()
            l_copy(j, 2, 3).wait_send()

            @pl.loop(0, nc)
            def _(c):
                o_copy(c, j, 1, 2).wait_send()
                o_copy(c, j, 2, 3).wait_send()

    @pl.when(z == 2)
    def _():
        for d in range(nt):
            far(d, 1, 0, 1).wait_send()
        for j in range(2):
            l_copy(j, 1, 3).wait_send()

            @pl.loop(0, nc)
            def _(c):
                q_copy(c, j, 1, 1).wait_send()
                o_copy(c, j, 1, 3).wait_send()

    @pl.when(z == 3)
    def _():
        for d in range(nt):
            far(d, 2, 0, 1).wait_send()
            far(d, 2, 1, 2).wait_send()
        for j in range(2):

            @pl.loop(0, nc)
            def _(c):
                q_copy(c, j, 2, 1).wait_send()
                q_copy(c, j, 1, 2).wait_send()

    _t.__exit__(None, None, None)


def fused(ns, nt, tokens, w_query, w_key, w_value, w_out, gain_query, gain_key):
    tok, seqs, depth = tokens.shape
    local = w_query.shape[1]
    nc = local // COLS
    oc = 1024
    no = depth // oc
    rows = tok * seqs
    width = HEADS * HEAD_DIM
    vm = pltpu.VMEM
    dma = pltpu.SemaphoreType.DMA
    scratch = [
        vm((RING, depth, COLS), BF16), vm((no, local, oc), BF16),
        vm((tok, seqs, depth), BF16), vm((rows, depth), BF16), vm((rows, depth), BF16),
        vm((rows, HEAD_DIM), F32), vm((rows, HEAD_DIM), F32), vm((2, nc, 1, COLS), F32), vm((2, rows, HEAD_DIM), F32),
        vm((2, 8, rows), F32), vm((2, nt - 1, 8, rows), F32), vm((3, nt, 8, rows), F32),
        vm((3, rows, rows), F32), vm((2, 8, rows), F32),
        vm((2, nc, seqs, 3 * tok, COLS), BF16), vm((nc, seqs, 2 * tok, COLS), BF16),
        vm((nc, seqs, tok, COLS), F32), vm((seqs, tok, HEAD_DIM), F32),
        vm((2, nc, seqs, tok, COLS), BF16), vm((seqs, 2, tok, HEAD_DIM), F32), vm((seqs, 16, rows), F32),
        vm((2, nc, seqs, tok, COLS), BF16), vm((2, seqs, 16, rows), F32), vm((3, tok, HEAD_DIM), F32),
        vm((rows, local), BF16), vm((no, seqs, tok, oc), BF16), vm((nt - 1, no, seqs, tok // nt, oc), BF16),
        dma, dma((RING,)), dma((no,)), dma((2, nt - 1)), dma((2, nt - 1)), dma((2, nt)), dma((3, nt)),
        dma((2, nc)), dma((2, nc)), dma((2, nc)), dma((2, nc)),
        dma((2, 2, nc)), dma((2, 2, nc)), dma((2, 2, nc)), dma((2, 2, nc)), dma((2, 2)), dma((2, 2)),
        dma((nt - 1, 2, no)), dma((nt - 1, 2, no)),
    ]
    in_vmem = pl.BlockSpec(memory_space=pltpu.VMEM)
    anywhere = pl.BlockSpec(memory_space=pl.ANY)
    return pl.pallas_call(
        functools.partial(block_kernel, ns, nt, tok, width),
        out_shape=jax.ShapeDtypeStruct((tok // nt, seqs, depth), BF16),
        in_specs=[anywhere] + [in_vmem] * 2 + [anywhere] * 4,
        out_specs=in_vmem,
        scratch_shapes=scratch,
        compiler_params=pltpu.CompilerParams(collective_id=0, has_side_effects=True, vmem_limit_bytes=60 * 1024 * 1024),
    )(tokens, gain_query, gain_key, w_query, w_key, w_value, w_out)


def rotary(field, positions):
    half = HEAD_DIM // 2
    shaped = field.reshape(field.shape[0], -1, HEAD_DIM)
    freqs = jnp.exp(-jnp.log(500000.0) * jnp.arange(half, dtype=jnp.float32) * 2.0 / HEAD_DIM)
    angle = positions.astype(jnp.float32)[:, None] * freqs[None, :]
    cosine = jnp.cos(angle)[:, None, :]
    sine = jnp.sin(angle)[:, None, :]
    first = shaped[..., :half]
    second = shaped[..., half:]
    turned = jnp.concatenate(
        [first * cosine - second * sine, second * cosine + first * sine], axis=-1
    )
    return turned.reshape(field.shape[0], -1)


def local(tokens, w_query, w_key, w_value, w_out, gain_query, gain_key):
    tok_rows = tokens.shape[0]
    seq_count = tokens.shape[1]
    local_width = w_query.shape[1]
    local_heads = local_width // HEAD_DIM
    width = HEADS * HEAD_DIM
    flat = tokens.reshape(tok_rows * seq_count, tokens.shape[2])
    query = jnp.dot(flat, w_query, preferred_element_type=jnp.float32)
    key_raw = jnp.dot(flat, w_key, preferred_element_type=jnp.float32)
    sum_query, sum_key = lax.psum(
        (jnp.sum(query * query, axis=1), jnp.sum(key_raw * key_raw, axis=1)), "tensor"
    )
    value = jnp.dot(flat, w_value, preferred_element_type=jnp.float32).astype(jnp.bfloat16)
    scale_q = lax.rsqrt(sum_query / width + 1e-06)
    scale_k = lax.rsqrt(sum_key / width + 1e-06)
    my_block = lax.axis_index("seq")
    positions = my_block * tok_rows + jnp.arange(tok_rows, dtype=jnp.int32)
    row_positions = (positions[:, None] + jnp.zeros((1, seq_count), jnp.int32)).reshape(-1)
    q_normed = rotary(query * scale_q[:, None] * gain_query[None, :], row_positions).astype(
        jnp.bfloat16
    )
    k_normed = rotary(key_raw * scale_k[:, None] * gain_key[None, :], row_positions).astype(
        jnp.bfloat16
    )
    q_heads = q_normed.reshape(tok_rows, seq_count, local_heads, HEAD_DIM)
    k_local = k_normed.reshape(tok_rows, seq_count, local_width)
    v_local = value.reshape(tok_rows, seq_count, local_width)
    factor = HEAD_DIM ** (-0.5)
    piece = (
        lax.all_gather(k_local, "seq", axis=0, tiled=True),
        lax.all_gather(v_local, "seq", axis=0, tiled=True),
    )
    key_pos = jnp.arange(piece[0].shape[0], dtype=jnp.int32)
    key_block = piece[0]
    count = key_block.shape[0]
    key_heads = key_block.reshape(count, seq_count, local_heads, HEAD_DIM)
    value_heads = piece[1].reshape(count, seq_count, local_heads, HEAD_DIM)
    scores = (
        jnp.einsum("qshd,kshd->shqk", q_heads, key_heads, preferred_element_type=jnp.float32)
        * factor
    )
    allowed = (key_pos[None, None, None, :] <= positions[None, None, :, None]) & (
        key_pos[None, None, None, :] >= 0
    )
    old_max = jnp.full((seq_count, local_heads, tok_rows), -1e30, jnp.float32)
    new_max = jnp.maximum(old_max, jnp.max(jnp.where(allowed, scores, -1e30), axis=3))
    expo = jnp.where(allowed, jnp.exp(scores - new_max[..., None]), 0.0)
    new_total = jnp.sum(expo, axis=3)
    added = jnp.einsum(
        "shqk,kshd->shqd",
        expo.astype(jnp.bfloat16),
        value_heads,
        preferred_element_type=jnp.float32,
    )
    final_state = (new_max, new_total, added)
    final_max, final_total, final_acc = final_state
    mixed = (final_acc / final_total[..., None]).astype(jnp.bfloat16)
    mixed = jnp.transpose(mixed, (2, 0, 1, 3)).reshape(tok_rows, seq_count, local_width)
    return lax.psum_scatter(
        jnp.dot(mixed, w_out, preferred_element_type=jnp.float32).astype(jnp.bfloat16),
        "tensor",
        scatter_dimension=0,
        tiled=True,
    )


def solution(mesh):
    ns, nt = mesh.shape["seq"], mesh.shape["tensor"]
    step = functools.partial(fused, ns, nt) if ns == 4 and nt == 4 else local
    return jax.shard_map(
        step,
        mesh=mesh,
        in_specs=(
            P("seq", "dp", None),
            P(None, "tensor"),
            P(None, "tensor"),
            P(None, "tensor"),
            P("tensor", None),
            P("tensor"),
            P("tensor"),
        ),
        out_specs=P(("seq", "tensor"), "dp", None),
        check_vma=False,
    )
```

```python
import contextlib
import functools

import jax
import jax.numpy as jnp
from jax import lax
from jax.experimental import pallas as pl
from jax.experimental.pallas import tpu as pltpu
from jax.sharding import PartitionSpec as P

HEADS = 40
HEAD_DIM = 128
MESH = pl.DeviceIdType.MESH
COLS = 2 * HEAD_DIM
RING = 9
LIFT = 1
F32 = jnp.float32
BF16 = jnp.bfloat16


def scope(name):
    return contextlib.nullcontext()


def block_kernel(
    ns, nt, tok, width,
    x_hbm, gq_hbm, gk_hbm, wq, wk, wv, wo,
    out_ref,
    gq_in, gk_in, ring, wov, xin, xi, xs, cos_ref, sin_ref, gains, ssq,
    sums_out, sums_in, sums_far, rqs, rks,
    qk, vbuf, own_o, own_lse, oout, lse_out, lse_msg, oin, lse_in, shares,
    mixed, part, rs_one, rs_mid, rs_two,
    x_sem, g_sem, w_sem, wo_sem, sum_send, sum_recv, far_send, far_recv, k_send, v_send, kv_recv,
    q_send, q_recv, o_send, o_recv, l_send, l_recv, one_send, one_recv, two_send, two_recv,
):
    dp = lax.axis_index("dp")
    z = lax.axis_index("seq")
    me = lax.axis_index("tensor")
    low = z < 2
    high = z >= 2
    nc = vbuf.shape[0]
    rows = 2 * tok
    oc = wov.shape[2]
    no = wov.shape[0]

    def w_copy(ref, c, slot):
        return pltpu.make_async_copy(
            ref.at[:, pl.ds(pl.multiple_of(c * COLS, COLS), COLS)], ring.at[slot], w_sem.at[slot]
        )

    def wo_copy(c):
        return pltpu.make_async_copy(
            wo.at[:, pl.ds(pl.multiple_of(c * oc, oc), oc)], wov.at[c], wo_sem.at[c]
        )

    def start(i):
        slot = lax.rem(i, RING)
        group = i // nc
        c = i - group * nc
        inside = i < 3 * nc

        @pl.when(inside & ((low & (group == 0)) | (high & (group == 1))))
        def _():
            w_copy(wk, c, slot).start()

        @pl.when(inside & ((low & (group == 1)) | (high & (group == 2))))
        def _():
            w_copy(wv, c, slot).start()

        @pl.when(inside & ((low & (group == 2)) | (high & (group == 0))))
        def _():
            w_copy(wq, c, slot).start()

        @pl.when((i >= 3 * nc) & (i < 3 * nc + no))
        def _():
            wo_copy(i - 3 * nc).start()

    x_copy = pltpu.make_async_copy(x_hbm, xin, x_sem)
    x_copy.start()
    g_copies = [pltpu.make_async_copy(gk_hbm, gk_in, g_sem.at[0]), pltpu.make_async_copy(gq_hbm, gq_in, g_sem.at[1])]
    for copy in g_copies:
        copy.start()

    barrier = pltpu.get_barrier_semaphore()
    linked = {0: (1, 2), 1: (0, 2, 3), 2: (0, 1, 3), 3: (1, 2)}
    for d in range(1, nt):
        pl.semaphore_signal(barrier, inc=1, device_id=(dp, z, lax.rem(me + d, nt)), device_id_type=MESH)
    for a in range(ns):
        hit = functools.reduce(jnp.logical_or, [z == b for b in linked[a]])

        @pl.when(hit)
        def _():
            for d in range(nt):
                pl.semaphore_signal(barrier, inc=1, device_id=(dp, a, lax.rem(me + d, nt)), device_id_type=MESH)

    def greet():
        pl.semaphore_wait(barrier, nt - 1 + nt * jnp.where((z == 1) | (z == 2), 3, 2))

    def remote(src, dst, ssem, rsem, to):
        return pltpu.make_async_remote_copy(
            src_ref=src, dst_ref=dst, send_sem=ssem, recv_sem=rsem, device_id=to, device_id_type=MESH
        )

    def settle(ref, sem):
        pltpu.make_async_copy(ref, ref, sem).wait()

    def k_copy(c, j, b, to):
        at = b * tok
        return remote(qk.at[0, c, j, pl.ds(0, tok)], qk.at[0, c, j, pl.ds(at, tok)], k_send.at[to - 1], kv_recv.at[j, c], (dp, to, me))

    def v_copy(c, j, b, to):
        at = b * tok
        return remote(vbuf.at[c, j, pl.ds(0, tok)], vbuf.at[c, j, pl.ds(at, tok)], v_send.at[to - 1], kv_recv.at[j, c], (dp, to, me))

    def q_copy(c, j, s, to):
        return remote(qk.at[1, c, j, pl.ds(0, tok)], qk.at[1, c, j, pl.ds(s * tok, tok)], q_send.at[s - 1], q_recv.at[j, c], (dp, to, me))

    def o_copy(c, j, s, to):
        return remote(oout.at[s - 1, c, j], oin.at[s - 1, c, j], o_send.at[s - 1], o_recv.at[j, c], (dp, to, me))

    def l_copy(j, s, to):
        return remote(lse_msg.at[j], lse_in.at[s - 1, j], l_send.at[s - 1], l_recv.at[j], (dp, to, me))

    def near(g, d):
        return remote(sums_out.at[g], sums_in.at[g, d - 1], sum_send.at[g], sum_recv.at[g], (dp, z, lax.rem(me + d, nt)))

    def far(d, slot, ss, to):
        return remote(sums_out.at[0], sums_far.at[slot, d], far_send.at[ss], far_recv.at[slot], (dp, to, lax.rem(me + d, nt)))

    def product(i):
        slot = lax.rem(i, RING)
        start(i + RING - 1)
        with scope("wwait"):
            w_copy(wk, 0, slot).wait()
        return jnp.dot(xs[...], ring[slot], preferred_element_type=F32)

    def turned(acc, kind, c):
        cosine, sine = cos_ref[...], sin_ref[...]
        for h in range(2):
            y = acc[:, h * HEAD_DIM : (h + 1) * HEAD_DIM] * gains[kind, c, :, h * HEAD_DIM : (h + 1) * HEAD_DIM]
            y = (y * cosine + pltpu.roll(y, HEAD_DIM // 2, 1) * sine).astype(BF16)
            for j in range(2):
                qk[kind, c, j, 0:tok, h * HEAD_DIM : (h + 1) * HEAD_DIM] = y[j * tok : (j + 1) * tok]

    def finish(acc, kind, c):
        ssq[kind] += acc[:, :HEAD_DIM] * acc[:, :HEAD_DIM] + acc[:, HEAD_DIM:] * acc[:, HEAD_DIM:]
        turned(acc, kind, c)

    def keep_value(acc, c):
        v = acc.astype(BF16)
        for j in range(2):
            vbuf[c, j, 0:tok, :] = v[j * tok : (j + 1) * tok]

    with scope("init"):
        lanes = lax.broadcasted_iota(jnp.int32, (tok, HEAD_DIM), 1)
        half = HEAD_DIM // 2
        freqs = jnp.exp(-jnp.log(500000.0) * lax.rem(lanes, half).astype(F32) * 2.0 / HEAD_DIM)
        spot = z * tok + lax.broadcasted_iota(jnp.int32, (tok, HEAD_DIM), 0)
        angle = spot.astype(F32) * freqs
        cosine = jnp.cos(angle)
        sine = jnp.sin(angle)
        sine = jnp.where(lanes < half, -sine, sine)
        for j in range(2):
            cos_ref[j * tok : (j + 1) * tok] = cosine
            sin_ref[j * tok : (j + 1) * tok] = sine

        @pl.loop(0, RING - 1)
        def _(i):
            start(i)

        for copy in g_copies:
            copy.wait()
        for c in range(nc):
            gains[0, c] = gk_in[c * COLS : (c + 1) * COLS].reshape(1, COLS)
            gains[1, c] = gq_in[c * COLS : (c + 1) * COLS].reshape(1, COLS)
        ssq[...] = jnp.zeros_like(ssq)
        sums_out[...] = jnp.zeros_like(sums_out)
        own_lse[...] = jnp.zeros_like(own_lse)
        lse_out[...] = jnp.full_like(lse_out, -1e30)

    with scope("xwait"):
        x_copy.wait()
    with scope("xlay"):
        @pl.loop(0, tok // 8)
        def _(i):
            v = xin[pl.ds(pl.multiple_of(i * 8, 8), 8)]
            xi[pl.ds(pl.multiple_of(i * 16, 16), 16), :] = v.reshape(16, v.shape[-1])

        r = lax.broadcasted_iota(jnp.int32, (rows, rows), 0)
        q = lax.broadcasted_iota(jnp.int32, (rows, rows), 1)
        pick = (q == jnp.where(r < tok, 2 * r, 2 * (r - tok) + 1)).astype(F32).astype(BF16)

        half_depth = xs.shape[1] // 2
        for i in range(2):
            at = slice(i * half_depth, (i + 1) * half_depth)
            xs[:, at] = jnp.dot(pick, xi[:, at], preferred_element_type=F32).astype(BF16)

    def fill_sums(g, kind):
        sums_out[g, 0:1, :] = jnp.sum(jnp.transpose(ssq[kind]), axis=0, keepdims=True)

    def send_near(g):
        for d in range(1, nt):
            near(g, d).start()

    def send_sums(g, kind):
        fill_sums(g, kind)
        send_near(g)

    first = jnp.where(low, 0, 1)

    with scope("g0"):
        @pl.loop(0, nc)
        def _(c):
            acc = product(c)

            @pl.when((c == 0) & ((z == 0) | (z == 3)))
            def _():
                greet()

            finish(acc, first, c)

            @pl.when((z == 0) & (c < LIFT))
            def _():
                k_copy(c, 0, 1, 2).start()

            @pl.when((z == 0) & (c >= LIFT))
            def _():
                k_copy(c, 0, 1, 1).start()

            @pl.when((z == 3) & (c < LIFT))
            def _():
                q_copy(c, 0, 1, 2).start()

            @pl.when((z == 3) & (c >= LIFT) & (c < nc - 2))
            def _():
                q_copy(c, 0, 2, 1).start()

    @pl.when((z == 1) | (z == 2))
    def _():
        with scope("barwait"):
            greet()

    fill_sums(0, first)

    @pl.when(z == 0)
    def _():
        for to in (1, 2):
            for d in range(nt):
                far(d, 0, to - 1, to).start()

    @pl.when(z == 1)
    def _():
        for d in range(nt):
            far(d, 1, 0, 2).start()

    @pl.when(z == 2)
    def _():
        for d in range(nt):
            far(d, 1, 0, 1).start()

    @pl.when(z == 3)
    def _():
        for to in (1, 2):
            for d in range(nt):
                far(d, 2, to - 1, to).start()

    send_near(0)

    @pl.when(z == 3)
    def _():
        @pl.loop(nc - 2, nc)
        def _(c):
            q_copy(c, 0, 2, 1).start()

    @pl.when(z == 1)
    def _():
        @pl.loop(0, LIFT)
        def _(c):
            for j in range(2):
                k_copy(c, j, 2, 2).start()

    with scope("g1"):
        @pl.loop(0, nc)
        def _(c):
            acc = product(nc + c)

            @pl.when(low)
            def _():
                keep_value(acc, c)

            @pl.when(high)
            def _():
                finish(acc, 0, c)

            @pl.when((z == 0) & (c < LIFT))
            def _():
                v_copy(c, 0, 1, 2).start()

            @pl.when((z == 0) & (c >= LIFT))
            def _():
                v_copy(c, 0, 1, 1).start()

            @pl.when((z == 1) & (c < LIFT))
            def _():
                for j in range(2):
                    v_copy(c, j, 2, 2).start()

            @pl.when((z == 2) & (c >= LIFT))
            def _():
                q_copy(c, 0, 1, 1).start()

            @pl.when((z == 3) & (c >= LIFT))
            def _():
                q_copy(c, 0, 1, 2).start()

            @pl.when((z == 3) & (c < LIFT))
            def _():
                q_copy(c, 1, 1, 2).start()

    @pl.when(high)
    def _():
        send_sums(1, 0)

    def near_scale(g):
        settle(sums_in.at[g], sum_recv.at[g])
        tot = sums_out[g]
        for d in range(1, nt):
            tot = tot + sums_in[g, d - 1]
        return lax.rsqrt(tot / width + 1e-06)

    def far_scale(slot):
        settle(sums_far.at[slot], far_recv.at[slot])
        tot = sums_far[slot, 0]
        for d in range(1, nt):
            tot = tot + sums_far[slot, d]
        return lax.rsqrt(tot / width + 1e-06)

    def set_rq(s, r):
        rqs[s] = jnp.transpose(jnp.broadcast_to(r[0:1, :] * HEAD_DIM ** (-0.5), (2 * rows, rows)))

    def set_rk(r0, r1, r2=None):
        left = lax.broadcasted_iota(jnp.int32, r0.shape, 1) < tok
        rks[0, :, 0:rows] = jnp.where(left, r0, pltpu.roll(r1, tok, 1))
        rks[1, :, 0:rows] = jnp.where(left, pltpu.roll(r0, tok, 1), r1)
        if r2 is not None:
            rks[0, :, rows : 2 * rows] = r2
            rks[1, :, rows : 2 * rows] = pltpu.roll(r2, tok, 1)

    lane = lax.broadcasted_iota(jnp.int32, (tok, HEAD_DIM), 1)

    def attend(c, js, lo, hi, nk, whole):
        row = lax.broadcasted_iota(jnp.int32, (tok, nk * tok), 0)
        col = lax.broadcasted_iota(jnp.int32, (tok, nk * tok), 1)
        allowed = (col <= row) | (col >= tok)
        units = [(j, h, slice(h * HEAD_DIM, (h + 1) * HEAD_DIM)) for j in js for h in range(2)]
        spans = range(lo, hi)
        scores = [
            lax.dot_general(
                qk[1, c, j, lo * tok : hi * tok, hs], qk[0, c, j, 0 : nk * tok, hs],
                (((1,), (1,)), ((), ())), preferred_element_type=F32,
            )
            for j, h, hs in units
        ]
        scaled = []
        for (j, h, hs), score in zip(units, scores):
            for s in spans:
                sc = score[(s - lo) * tok : (s - lo + 1) * tok]
                sc = sc * rqs[s, j * tok : (j + 1) * tok, 0 : nk * tok] * rks[j, 0:1, 0 : nk * tok]
                scaled.append(jnp.where(allowed, sc, -1e30) if s == 0 else sc)
        tops = [jnp.max(sc, axis=1, keepdims=True) for sc in scaled]
        expos = [jnp.exp(sc - top) for sc, top in zip(scaled, tops)]
        tots = [jnp.sum(e, axis=1, keepdims=True) for e in expos]
        n = hi - lo
        accs = []
        for i, (j, h, hs) in enumerate(units):
            w = [e.astype(BF16) for e in expos[i * n : (i + 1) * n]]
            w = w[0] if n == 1 else jnp.concatenate(w, axis=0)
            accs.append(jnp.dot(w, vbuf[c, j, 0 : nk * tok, hs], preferred_element_type=F32))
        for i, (j, h, hs) in enumerate(units):
            for s in spans:
                o = accs[i][(s - lo) * tok : (s - lo + 1) * tok] / tots[i * n + s - lo]
                if s == 0 and whole:
                    mixed[j * tok : (j + 1) * tok, pl.ds(pl.multiple_of(c * COLS + h * HEAD_DIM, HEAD_DIM), HEAD_DIM)] = o.astype(BF16)
                elif s == 0:
                    own_o[c, j, :, hs] = o
                else:
                    oout[s - 1, c, j, :, hs] = o.astype(BF16)
        for i, j in enumerate(js):
            for s in spans:
                if s == 0 and whole:
                    continue
                a, b = (tops[u] + jnp.log(tots[u]) for u in (2 * i * n + s - lo, (2 * i + 1) * n + s - lo))
                if s > 0:
                    lse_out[j, s - 1] = jnp.where(lane == 2 * c, a, jnp.where(lane == 2 * c + 1, b, lse_out[j, s - 1]))
                else:
                    own_lse[j] = jnp.where(lane == 2 * c, a, jnp.where(lane == 2 * c + 1, b, own_lse[j]))

    def remote_part(c, j):
        @pl.when(z == 1)
        def _():
            with scope("attwait"):
                settle(qk.at[1, c, :, pl.ds(0, tok)], q_recv.at[j, c])
                settle(qk.at[0, c, :, pl.ds(0, tok)], kv_recv.at[j, c])
            attend(c, (j,), 1, 3, 2, False)
            o_copy(c, j, 2, 3).start()
            o_copy(c, j, 1, 2).start()

        @pl.when(z == 2)
        def _():
            with scope("attwait"):
                settle(qk.at[1, c, j, pl.ds(0, tok)], q_recv.at[j, c])
            attend(c, (j,), 0, 2, 1, False)
            o_copy(c, j, 1, 3).start()

    def lifted_part(c, j):
        with scope("liftwait"):
            settle(qk.at[1, c, j, pl.ds(0, tok)], q_recv.at[j, c])
            settle(qk.at[0, c, :, pl.ds(0, 2 * tok)], kv_recv.at[j, c])
        attend(c, (j,), 0, 2, 3, True)
        o_copy(c, j, 1, 3).start()

    def send_lse(j):
        def message(a, b):
            lse_msg[j] = jnp.transpose(jnp.concatenate([a, b], axis=0))[0:16]

        @pl.when(z == 1)
        def _():
            message(lse_out[j, 0], lse_out[j, 1])
            l_copy(j, 2, 3).start()
            l_copy(j, 1, 2).start()

        @pl.when(z == 2)
        def _():
            message(lse_out[j, 0], lse_out[j, 0])
            l_copy(j, 1, 3).start()

    with scope("g2"):
        @pl.loop(0, nc)
        def _(c):
            acc = product(2 * nc + c)

            @pl.when(low)
            def _():
                finish(acc, 1, c)

            @pl.when(high)
            def _():
                keep_value(acc, c)

            @pl.when((z == 0) & (c >= LIFT))
            def _():
                k_copy(c, 1, 1, 1).start()
                v_copy(c, 1, 1, 1).start()

            @pl.when((z == 2) & (c >= LIFT))
            def _():
                q_copy(c, 1, 1, 1).start()

            @pl.when((z == 3) & (c >= LIFT))
            def _():
                q_copy(c, 1, 2, 1).start()
                q_copy(c, 1, 1, 2).start()

            @pl.when((c == LIFT) & (z == 1))
            def _():
                with scope("sw_near"):
                    a = near_scale(0)
                with scope("sw_far0"):
                    set_rk(a, far_scale(0))
                with scope("sw_far1"):
                    set_rq(1, far_scale(1))
                with scope("sw_far2"):
                    set_rq(2, far_scale(2))

            @pl.when((z == 1) & (c >= LIFT))
            def _():
                remote_part(c, 0)

    @pl.when(z == 0)
    def _():
        @pl.loop(0, LIFT)
        def _(c):
            k_copy(c, 1, 1, 2).start()
            v_copy(c, 1, 1, 2).start()

        @pl.loop(0, LIFT)
        def _(c):
            for j in range(2):
                k_copy(c, j, 1, 1).start()
                v_copy(c, j, 1, 1).start()

    @pl.when(low)
    def _():
        send_sums(1, 1)

    @pl.when(high)
    def _():
        with scope("sw_near"):
            set_rq(0, near_scale(0))
            r = near_scale(1)

        @pl.when(z == 3)
        def _():
            set_rk(r, r)

        @pl.when(z == 2)
        def _():
            with scope("sw_far"):
                set_rk(r, far_scale(0), far_scale(1))
                set_rq(1, far_scale(2))

    with scope("rem0"):
        @pl.when(z == 2)
        def _():
            @pl.loop(LIFT, nc)
            def _(c):
                remote_part(c, 0)

            @pl.loop(0, LIFT)
            def _(c):
                lifted_part(c, 0)

        send_lse(0)

    with scope("rem1"):
        @pl.when((z == 1) | (z == 2))
        def _():
            @pl.loop(LIFT, nc)
            def _(c):
                remote_part(c, 1)

        @pl.when(z == 2)
        def _():
            @pl.loop(0, LIFT)
            def _(c):
                lifted_part(c, 1)

        send_lse(1)

    @pl.when(z == 0)
    def _():
        with scope("own"):
            r = near_scale(0)
            set_rk(r, r)
            set_rq(0, near_scale(1))

            @pl.loop(0, nc)
            def _(c):
                attend(c, (0, 1), 0, 1, 1, True)

    @pl.when(z == 1)
    def _():
        with scope("own"):
            set_rq(0, near_scale(1))

            @pl.loop(0, nc)
            def _(i):
                c = lax.rem(i + LIFT, nc)

                @pl.when(c < LIFT)
                def _():
                    with scope("ownwait"):
                        for j in range(2):
                            settle(qk.at[0, c, :, pl.ds(0, tok)], kv_recv.at[j, c])

                attend(c, (0, 1), 0, 1, 2, True)

    @pl.when(z == 3)
    def _():
        with scope("own"):
            @pl.loop(0, nc)
            def _(c):
                attend(c, (0, 1), 0, 1, 1, False)

    def merge(j, ni):
        lses = [own_lse[j]]
        settle(lse_in.at[pl.ds(0, ni), j], l_recv.at[j])
        for s in range(1, ni + 1):
            wide = jnp.concatenate([lse_in[s - 1, j], jnp.zeros((rows - 16, rows), F32)], axis=0)
            lses.append(jnp.transpose(wide)[(ni - 1) * tok : ni * tok])
        top = functools.reduce(jnp.maximum, lses)
        parts = [jnp.exp(v - top) for v in lses]
        tot = functools.reduce(jnp.add, parts)
        for s in range(ni + 1):
            shares[s] = parts[s] / tot

        def blend(c, count):
            settle(oin.at[pl.ds(0, count), c, j], o_recv.at[j, c])
            for h in range(2):
                hs = slice(h * HEAD_DIM, (h + 1) * HEAD_DIM)
                o = 0.0
                for s in range(count + 1):
                    share = jnp.sum(jnp.where(lane == 2 * c + h, shares[s], 0.0), axis=1, keepdims=True)
                    o += share * (own_o[c, j, :, hs] if s == 0 else oin[s - 1, c, j, :, hs].astype(F32))
                mixed[j * tok : (j + 1) * tok, pl.ds(pl.multiple_of(c * COLS + h * HEAD_DIM, HEAD_DIM), HEAD_DIM)] = o.astype(BF16)

        if ni == 2:
            @pl.loop(0, LIFT)
            def _(c):
                blend(c, 1)

        @pl.loop(LIFT, nc)
        def _(c):
            blend(c, ni)

    share = tok // nt
    hc = oc // 2
    my, mx = me // 2, lax.rem(me, 2)

    def stage_one(n, j, half):
        if half == 0:
            src, to = part.at[n, j, half, :, 1 - mx], 2 * my + 1 - mx
        else:
            src, to = part.at[n, j, half, 1 - my], 2 * (1 - my) + mx
        return remote(src, rs_one.at[n, j, half], one_send, one_recv.at[j, n], (dp, z, to))

    def stage_two(n, j, half):
        to = 2 * (1 - my) + mx if half == 0 else 2 * my + 1 - mx
        return remote(rs_mid.at[n, j, half], rs_two.at[n, j, half], two_send, two_recv.at[j, n], (dp, z, to))

    def project(js, first_pass):
        lo, hi = js[0] * tok, (js[-1] + 1) * tok

        @pl.loop(0, no)
        def _(n):
            if first_pass:
                wo_copy(n).wait()
            acc = jnp.dot(mixed[lo:hi], wov[n], preferred_element_type=F32).astype(BF16)
            for j in js:
                for half in range(2):
                    for t in range(nt):
                        row = j * tok + t * share - lo
                        part[n, j, half, t // 2, t % 2] = acc[row : row + share, half * hc : (half + 1) * hc]
                    stage_one(n, j, half).start()

    def forward(j):
        with scope("fwd"):
            @pl.loop(0, no)
            def _(n):
                settle(rs_one.at[n, j], one_recv.at[j, n])
                for half in range(2):
                    if half == 0:
                        o = part[n, j, half, 1 - my, mx].astype(F32) + rs_one[n, j, half, 1 - my].astype(F32)
                    else:
                        o = part[n, j, half, my, 1 - mx].astype(F32) + rs_one[n, j, half, 1 - mx].astype(F32)
                    rs_mid[n, j, half] = o.astype(BF16)
                    stage_two(n, j, half).start()

    def collect(j):
        with scope("collect"):
            @pl.loop(0, no)
            def _(n):
                settle(rs_two.at[n, j], two_recv.at[j, n])
                for half in range(2):
                    o = part[n, j, half, my, mx].astype(F32) + rs_one[n, j, half, my if half == 0 else mx].astype(F32)
                    o = o + rs_two[n, j, half].astype(F32)
                    out_ref[:, j, pl.ds(pl.multiple_of(n * oc + half * hc, hc), hc)] = o.astype(BF16)

    @pl.when(low)
    def _():
        with scope("outp"):
            project((0, 1), True)

    @pl.when(high)
    def _():
        for j in range(2):
            with scope("merge"):
                @pl.when(z == 2)
                def _():
                    merge(j, 1)

                @pl.when(z == 3)
                def _():
                    merge(j, 2)

            with scope("outp"):
                project((j,), j == 0)

    for j in range(2):
        forward(j)
    for j in range(2):
        collect(j)

    _t = scope("tail")
    _t.__enter__()
    settle(rs_one, one_send)
    settle(rs_mid, two_send)
    for g in range(2):
        settle(sums_in.at[g], sum_send.at[g])

    lifted, others = pl.ds(0, LIFT), pl.ds(LIFT, nc - LIFT)
    own_rows = pl.ds(0, tok)

    @pl.when(z == 0)
    def _():
        for i, part_of in enumerate((pl.ds(0, nc), lifted)):
            settle(sums_far.at[0], far_send.at[i])
            settle(qk.at[0, part_of, :, own_rows], k_send.at[i])
            settle(vbuf.at[part_of, :, own_rows], v_send.at[i])

    @pl.when(z == 1)
    def _():
        settle(sums_far.at[0], far_send.at[0])
        settle(qk.at[0, lifted, :, own_rows], k_send.at[1])
        settle(vbuf.at[lifted, :, own_rows], v_send.at[1])
        for i in range(2):
            settle(lse_msg, l_send.at[i])
            settle(oout.at[i, others], o_send.at[i])

    @pl.when(z == 2)
    def _():
        settle(sums_far.at[0], far_send.at[0])
        settle(lse_msg, l_send.at[0])
        settle(oout.at[0], o_send.at[0])
        settle(qk.at[1, others, :, own_rows], q_send.at[0])

    @pl.when(z == 3)
    def _():
        for i in range(2):
            settle(sums_far.at[0], far_send.at[i])
        settle(qk.at[1, :, :, own_rows], q_send.at[0])
        settle(qk.at[1, others, :, own_rows], q_send.at[1])

    _t.__exit__(None, None, None)


def fused(ns, nt, tokens, w_query, w_key, w_value, w_out, gain_query, gain_key):
    tok, seqs, depth = tokens.shape
    local = w_query.shape[1]
    nc = local // COLS
    oc = 1024
    no = depth // oc
    rows = tok * seqs
    width = HEADS * HEAD_DIM
    vm = pltpu.VMEM
    dma = pltpu.SemaphoreType.DMA
    scratch = [
        vm((local,), F32), vm((local,), F32),
        vm((RING, depth, COLS), BF16), vm((no, local, oc), BF16),
        vm((tok, seqs, depth), BF16), vm((rows, depth), BF16), vm((rows, depth), BF16),
        vm((rows, HEAD_DIM), F32), vm((rows, HEAD_DIM), F32), vm((2, nc, 1, COLS), F32), vm((2, rows, HEAD_DIM), F32),
        vm((2, 8, rows), F32), vm((2, nt - 1, 8, rows), F32), vm((3, nt, 8, rows), F32),
        vm((3, rows, 2 * rows), F32), vm((2, 8, 2 * rows), F32),
        vm((2, nc, seqs, 3 * tok, COLS), BF16), vm((nc, seqs, 3 * tok, COLS), BF16),
        vm((nc, seqs, tok, COLS), F32), vm((seqs, tok, HEAD_DIM), F32),
        vm((2, nc, seqs, tok, COLS), BF16), vm((seqs, 2, tok, HEAD_DIM), F32), vm((seqs, 16, rows), F32),
        vm((2, nc, seqs, tok, COLS), BF16), vm((2, seqs, 16, rows), F32), vm((3, tok, HEAD_DIM), F32),
        vm((rows, local), BF16), vm((no, seqs, 2, 2, 2, tok // nt, oc // 2), BF16),
        vm((no, seqs, 2, 2, tok // nt, oc // 2), BF16), vm((no, seqs, 2, tok // nt, oc // 2), BF16), vm((no, seqs, 2, tok // nt, oc // 2), BF16),
        dma, dma((2,)), dma((RING,)), dma((no,)), dma((2,)), dma((2,)), dma((2,)), dma((3,)), dma((2,)), dma((2,)), dma((2, nc)),
        dma((2,)), dma((2, nc)), dma((2,)), dma((2, nc)), dma((2,)), dma((2,)), dma, dma((2, no)), dma, dma((2, no)),
    ]
    in_vmem = pl.BlockSpec(memory_space=pltpu.VMEM)
    in_hbm = pl.BlockSpec(memory_space=pltpu.HBM)
    return pl.pallas_call(
        functools.partial(block_kernel, ns, nt, tok, width),
        out_shape=pltpu.VMEM((tok // nt, seqs, depth), BF16),
        in_specs=[in_hbm] * 7,
        out_specs=in_vmem,
        scratch_shapes=scratch,
        compiler_params=pltpu.CompilerParams(collective_id=0, has_side_effects=True, vmem_limit_bytes=58 * 1024 * 1024),
    )(tokens, gain_query, gain_key, w_query, w_key, w_value, w_out)


def rotary(field, positions):
    half = HEAD_DIM // 2
    shaped = field.reshape(field.shape[0], -1, HEAD_DIM)
    freqs = jnp.exp(-jnp.log(500000.0) * jnp.arange(half, dtype=jnp.float32) * 2.0 / HEAD_DIM)
    angle = positions.astype(jnp.float32)[:, None] * freqs[None, :]
    cosine = jnp.cos(angle)[:, None, :]
    sine = jnp.sin(angle)[:, None, :]
    first = shaped[..., :half]
    second = shaped[..., half:]
    turned = jnp.concatenate(
        [first * cosine - second * sine, second * cosine + first * sine], axis=-1
    )
    return turned.reshape(field.shape[0], -1)


def local(tokens, w_query, w_key, w_value, w_out, gain_query, gain_key):
    tok_rows = tokens.shape[0]
    seq_count = tokens.shape[1]
    local_width = w_query.shape[1]
    local_heads = local_width // HEAD_DIM
    width = HEADS * HEAD_DIM
    flat = tokens.reshape(tok_rows * seq_count, tokens.shape[2])
    query = jnp.dot(flat, w_query, preferred_element_type=jnp.float32)
    key_raw = jnp.dot(flat, w_key, preferred_element_type=jnp.float32)
    sum_query, sum_key = lax.psum(
        (jnp.sum(query * query, axis=1), jnp.sum(key_raw * key_raw, axis=1)), "tensor"
    )
    value = jnp.dot(flat, w_value, preferred_element_type=jnp.float32).astype(jnp.bfloat16)
    scale_q = lax.rsqrt(sum_query / width + 1e-06)
    scale_k = lax.rsqrt(sum_key / width + 1e-06)
    my_block = lax.axis_index("seq")
    positions = my_block * tok_rows + jnp.arange(tok_rows, dtype=jnp.int32)
    row_positions = (positions[:, None] + jnp.zeros((1, seq_count), jnp.int32)).reshape(-1)
    q_normed = rotary(query * scale_q[:, None] * gain_query[None, :], row_positions).astype(
        jnp.bfloat16
    )
    k_normed = rotary(key_raw * scale_k[:, None] * gain_key[None, :], row_positions).astype(
        jnp.bfloat16
    )
    q_heads = q_normed.reshape(tok_rows, seq_count, local_heads, HEAD_DIM)
    k_local = k_normed.reshape(tok_rows, seq_count, local_width)
    v_local = value.reshape(tok_rows, seq_count, local_width)
    factor = HEAD_DIM ** (-0.5)
    piece = (
        lax.all_gather(k_local, "seq", axis=0, tiled=True),
        lax.all_gather(v_local, "seq", axis=0, tiled=True),
    )
    key_pos = jnp.arange(piece[0].shape[0], dtype=jnp.int32)
    key_block = piece[0]
    count = key_block.shape[0]
    key_heads = key_block.reshape(count, seq_count, local_heads, HEAD_DIM)
    value_heads = piece[1].reshape(count, seq_count, local_heads, HEAD_DIM)
    scores = (
        jnp.einsum("qshd,kshd->shqk", q_heads, key_heads, preferred_element_type=jnp.float32)
        * factor
    )
    allowed = (key_pos[None, None, None, :] <= positions[None, None, :, None]) & (
        key_pos[None, None, None, :] >= 0
    )
    old_max = jnp.full((seq_count, local_heads, tok_rows), -1e30, jnp.float32)
    new_max = jnp.maximum(old_max, jnp.max(jnp.where(allowed, scores, -1e30), axis=3))
    expo = jnp.where(allowed, jnp.exp(scores - new_max[..., None]), 0.0)
    new_total = jnp.sum(expo, axis=3)
    added = jnp.einsum(
        "shqk,kshd->shqd",
        expo.astype(jnp.bfloat16),
        value_heads,
        preferred_element_type=jnp.float32,
    )
    final_state = (new_max, new_total, added)
    final_max, final_total, final_acc = final_state
    mixed = (final_acc / final_total[..., None]).astype(jnp.bfloat16)
    mixed = jnp.transpose(mixed, (2, 0, 1, 3)).reshape(tok_rows, seq_count, local_width)
    return lax.psum_scatter(
        jnp.dot(mixed, w_out, preferred_element_type=jnp.float32).astype(jnp.bfloat16),
        "tensor",
        scatter_dimension=0,
        tiled=True,
    )


def solution(mesh):
    ns, nt = mesh.shape["seq"], mesh.shape["tensor"]
    step = functools.partial(fused, ns, nt) if ns == 4 and nt == 4 else local
    return jax.shard_map(
        step,
        mesh=mesh,
        in_specs=(
            P("seq", "dp", None),
            P(None, "tensor"),
            P(None, "tensor"),
            P(None, "tensor"),
            P("tensor", None),
            P("tensor"),
            P("tensor"),
        ),
        out_specs=P(("seq", "tensor"), "dp", None),
        check_vma=False,
    )
```

```python
import contextlib
import functools

import jax
import jax.numpy as jnp
from jax import lax
from jax.experimental import pallas as pl
from jax.experimental.pallas import tpu as pltpu
from jax.sharding import PartitionSpec as P

HEADS = 40
HEAD_DIM = 128
MESH = pl.DeviceIdType.MESH
COLS = 2 * HEAD_DIM
RING = 9
LIFT = (1, 1)
F32 = jnp.float32
BF16 = jnp.bfloat16


def scope(name):
    return contextlib.nullcontext()


def block_kernel(
    ns, nt, tok, width,
    x_hbm, gq_hbm, gk_hbm, wq, wk, wv, wo,
    out_ref,
    gq_in, gk_in, ring, wov, xin, xi, xs, cos_ref, sin_ref, gains, ssq,
    sums_out, sums_in, sums_far, rqs, rks,
    qk, vbuf, own_o, own_lse, oout, lse_out, lse_msg, oin, lse_in, shares,
    mixed, part, rs_one, rs_mid, rs_two,
    x_sem, g_sem, w_sem, wo_sem, sum_send, sum_recv, far_send, far_recv, k_send, v_send, kv_recv,
    q_send, q_recv, o_send, o_recv, l_send, l_recv, one_send, one_recv, two_send, two_recv,
):
    dp = lax.axis_index("dp")
    z = lax.axis_index("seq")
    me = lax.axis_index("tensor")
    low = z < 2
    high = z >= 2
    nc = vbuf.shape[0]
    rows = 2 * tok
    oc = wov.shape[2]
    no = wov.shape[0]

    def w_copy(ref, c, slot):
        return pltpu.make_async_copy(
            ref.at[:, pl.ds(pl.multiple_of(c * COLS, COLS), COLS)], ring.at[slot], w_sem.at[slot]
        )

    def wo_copy(c):
        return pltpu.make_async_copy(
            wo.at[:, pl.ds(pl.multiple_of(c * oc, oc), oc)], wov.at[c], wo_sem.at[c]
        )

    def start(i):
        slot = lax.rem(i, RING)
        group = i // nc
        c = i - group * nc
        inside = i < 3 * nc

        @pl.when(inside & ((low & (group == 0)) | (high & (group == 1))))
        def _():
            w_copy(wk, c, slot).start()

        @pl.when(inside & (((z == 0) & (group == 1)) | ((z > 0) & (group == 2))))
        def _():
            w_copy(wv, c, slot).start()

        @pl.when(inside & (((z == 0) & (group == 2)) | ((z == 1) & (group == 1)) | (high & (group == 0))))
        def _():
            w_copy(wq, c, slot).start()

        @pl.when((i >= 3 * nc) & (i < 3 * nc + no))
        def _():
            wo_copy(i - 3 * nc).start()

    x_copy = pltpu.make_async_copy(x_hbm, xin, x_sem)
    x_copy.start()
    g_copies = [pltpu.make_async_copy(gk_hbm, gk_in, g_sem.at[0]), pltpu.make_async_copy(gq_hbm, gq_in, g_sem.at[1])]
    for copy in g_copies:
        copy.start()

    barrier = pltpu.get_barrier_semaphore()
    linked = {0: (1, 2), 1: (0, 2, 3), 2: (0, 1, 3), 3: (1, 2)}
    for d in range(1, nt):
        pl.semaphore_signal(barrier, inc=1, device_id=(dp, z, lax.rem(me + d, nt)), device_id_type=MESH)
    for a in range(ns):
        hit = functools.reduce(jnp.logical_or, [z == b for b in linked[a]])

        @pl.when(hit)
        def _():
            for d in range(nt):
                pl.semaphore_signal(barrier, inc=1, device_id=(dp, a, lax.rem(me + d, nt)), device_id_type=MESH)

    def greet():
        pl.semaphore_wait(barrier, nt - 1 + nt * jnp.where((z == 1) | (z == 2), 3, 2))

    def remote(src, dst, ssem, rsem, to):
        return pltpu.make_async_remote_copy(
            src_ref=src, dst_ref=dst, send_sem=ssem, recv_sem=rsem, device_id=to, device_id_type=MESH
        )

    def settle(ref, sem):
        pltpu.make_async_copy(ref, ref, sem).wait()

    def blocks(count):
        return xi.at[:, pl.ds(0, count * HEAD_DIM)]

    def k_copy(c, j, b, to):
        at = b * tok
        return remote(qk.at[0, c, j, pl.ds(0, tok)], qk.at[0, c, j, pl.ds(at, tok)], k_send.at[to - 1], kv_recv.at[j, c], (dp, to, me))

    def v_copy(c, j, b, to):
        at = b * tok
        return remote(vbuf.at[c, j, pl.ds(0, tok)], vbuf.at[c, j, pl.ds(at, tok)], v_send.at[to - 1], kv_recv.at[j, c], (dp, to, me))

    def q_copy(c, j, s, to):
        return remote(qk.at[1, c, j, pl.ds(0, tok)], qk.at[1, c, j, pl.ds(s * tok, tok)], q_send.at[s - 1], q_recv.at[j, c], (dp, to, me))

    def o_copy(c, j, s, to):
        return remote(oout.at[s - 1, c, j], oin.at[s - 1, c, j], o_send.at[s - 1], o_recv.at[j, c], (dp, to, me))

    def l_copy(j, s, to):
        return remote(lse_msg.at[j], lse_in.at[s - 1, j], l_send.at[s - 1], l_recv.at[j], (dp, to, me))

    def near(g, d):
        return remote(sums_out.at[g], sums_in.at[g, d - 1], sum_send.at[g], sum_recv.at[g], (dp, z, lax.rem(me + d, nt)))

    def far(d, slot, ss, to, g=0):
        return remote(sums_out.at[g], sums_far.at[slot, d], far_send.at[ss], far_recv.at[slot], (dp, to, lax.rem(me + d, nt)))

    def product(i):
        slot = lax.rem(i, RING)
        start(i + RING - 1)
        with scope("wwait"):
            w_copy(wk, 0, slot).wait()
        return jnp.dot(xs[...], ring[slot], preferred_element_type=F32)

    def turned(acc, kind, c):
        cosine, sine = cos_ref[...], sin_ref[...]
        for h in range(2):
            y = acc[:, h * HEAD_DIM : (h + 1) * HEAD_DIM] * gains[kind, c, :, h * HEAD_DIM : (h + 1) * HEAD_DIM]
            y = (y * cosine + pltpu.roll(y, HEAD_DIM // 2, 1) * sine).astype(BF16)
            for j in range(2):
                qk[kind, c, j, 0:tok, h * HEAD_DIM : (h + 1) * HEAD_DIM] = y[j * tok : (j + 1) * tok]

    def finish(acc, kind, c):
        ssq[kind] += acc[:, :HEAD_DIM] * acc[:, :HEAD_DIM] + acc[:, HEAD_DIM:] * acc[:, HEAD_DIM:]
        turned(acc, kind, c)

    def keep_value(acc, c):
        v = acc.astype(BF16)
        for j in range(2):
            vbuf[c, j, 0:tok, :] = v[j * tok : (j + 1) * tok]

    with scope("init"):
        lanes = lax.broadcasted_iota(jnp.int32, (tok, HEAD_DIM), 1)
        half = HEAD_DIM // 2
        freqs = jnp.exp(-jnp.log(500000.0) * lax.rem(lanes, half).astype(F32) * 2.0 / HEAD_DIM)
        spot = z * tok + lax.broadcasted_iota(jnp.int32, (tok, HEAD_DIM), 0)
        angle = spot.astype(F32) * freqs
        cosine = jnp.cos(angle)
        sine = jnp.sin(angle)
        sine = jnp.where(lanes < half, -sine, sine)
        for j in range(2):
            cos_ref[j * tok : (j + 1) * tok] = cosine
            sin_ref[j * tok : (j + 1) * tok] = sine

        @pl.loop(0, RING - 1)
        def _(i):
            start(i)

        for copy in g_copies:
            copy.wait()
        for c in range(nc):
            gains[0, c] = gk_in[c * COLS : (c + 1) * COLS].reshape(1, COLS)
            gains[1, c] = gq_in[c * COLS : (c + 1) * COLS].reshape(1, COLS)
        ssq[...] = jnp.zeros_like(ssq)
        sums_out[...] = jnp.zeros_like(sums_out)
        own_lse[...] = jnp.zeros_like(own_lse)
        lse_out[...] = jnp.full_like(lse_out, -1e30)

    with scope("xwait"):
        x_copy.wait()
    with scope("xlay"):
        @pl.loop(0, tok // 8)
        def _(i):
            v = xin[pl.ds(pl.multiple_of(i * 8, 8), 8)]
            xi[pl.ds(pl.multiple_of(i * 16, 16), 16), :] = v.reshape(16, v.shape[-1])

        r = lax.broadcasted_iota(jnp.int32, (rows, rows), 0)
        q = lax.broadcasted_iota(jnp.int32, (rows, rows), 1)
        pick = (q == jnp.where(r < tok, 2 * r, 2 * (r - tok) + 1)).astype(F32).astype(BF16)

        half_depth = xs.shape[1] // 2
        for i in range(2):
            at = slice(i * half_depth, (i + 1) * half_depth)
            xs[:, at] = jnp.dot(pick, xi[:, at], preferred_element_type=F32).astype(BF16)

    def fill_sums(g, kind):
        sums_out[g, 0:1, :] = jnp.sum(jnp.transpose(ssq[kind]), axis=0, keepdims=True)

    def send_near(g):
        for d in range(1, nt):
            near(g, d).start()

    def send_sums(g, kind):
        fill_sums(g, kind)
        send_near(g)

    first = jnp.where(low, 0, 1)
    second = jnp.where(z == 1, 1, 0)

    with scope("g0"):
        @pl.loop(0, nc)
        def _(c):
            acc = product(c)

            @pl.when((c == 0) & ((z == 0) | (z == 3)))
            def _():
                greet()

            finish(acc, first, c)

            @pl.when((z == 0) & (c < LIFT[0]))
            def _():
                k_copy(c, 0, 1, 2).start()

            @pl.when((z == 0) & (c >= LIFT[0]))
            def _():
                k_copy(c, 0, 1, 1).start()

            @pl.when((z == 3) & (c < LIFT[0]))
            def _():
                q_copy(c, 0, 1, 2).start()

            @pl.when((z == 3) & (c >= LIFT[0]) & (c < nc - 2))
            def _():
                q_copy(c, 0, 2, 1).start()

    @pl.when((z == 1) | (z == 2))
    def _():
        with scope("barwait"):
            greet()

    fill_sums(0, first)

    @pl.when(z == 0)
    def _():
        for to in (1, 2):
            for d in range(nt):
                far(d, 0, to - 1, to).start()

    @pl.when(z == 1)
    def _():
        for d in range(nt):
            far(d, 1, 0, 2).start()

    @pl.when(z == 2)
    def _():
        for d in range(nt):
            far(d, 1, 0, 1).start()

    @pl.when(z == 3)
    def _():
        for to in (1, 2):
            for d in range(nt):
                far(d, 2, to - 1, to).start()

    send_near(0)

    @pl.when(z == 3)
    def _():
        @pl.loop(nc - 2, nc)
        def _(c):
            q_copy(c, 0, 2, 1).start()

    @pl.when(z == 1)
    def _():
        for j in range(2):

            @pl.loop(0, LIFT[j])
            def _(c):
                k_copy(c, j, 2, 2).start()

    with scope("g1"):
        @pl.loop(0, nc)
        def _(c):
            acc = product(nc + c)

            @pl.when(z == 0)
            def _():
                keep_value(acc, c)

            @pl.when(z > 0)
            def _():
                finish(acc, second, c)

            @pl.when((z == 0) & (c < LIFT[0]))
            def _():
                v_copy(c, 0, 1, 2).start()

            @pl.when((z == 0) & (c >= LIFT[0]))
            def _():
                v_copy(c, 0, 1, 1).start()

            @pl.when((z == 2) & (c >= LIFT[0]))
            def _():
                q_copy(c, 0, 1, 1).start()
                k_copy(c, 0, 1, 3).start()

            @pl.when((z == 3) & (c < LIFT[1]))
            def _():
                q_copy(c, 1, 1, 2).start()

    @pl.when(z > 0)
    def _():
        fill_sums(1, second)

        @pl.when(z == 2)
        def _():
            for d in range(nt):
                far(d, 0, 1, 3, 1).start()

        send_near(1)

    @pl.when(z == 0)
    def _():
        for j, to in ((1, 2), (0, 1)):

            @pl.loop(0, LIFT[j])
            def _(c):
                k_copy(c, j, 1, to).start()
                v_copy(c, j, 1, to).start()

    def near_scale(g):
        settle(sums_in.at[g], sum_recv.at[g])
        tot = sums_out[g]
        for d in range(1, nt):
            tot = tot + sums_in[g, d - 1]
        return lax.rsqrt(tot / width + 1e-06)

    def far_scale(slot):
        settle(sums_far.at[slot], far_recv.at[slot])
        tot = sums_far[slot, 0]
        for d in range(1, nt):
            tot = tot + sums_far[slot, d]
        return lax.rsqrt(tot / width + 1e-06)

    def set_rq(s, r):
        rqs[s] = jnp.transpose(jnp.broadcast_to(r[0:1, :] * HEAD_DIM ** (-0.5), (2 * rows, rows)))

    def set_rk(r0, r1, r2=None):
        left = lax.broadcasted_iota(jnp.int32, r0.shape, 1) < tok
        rks[0, :, 0:rows] = jnp.where(left, r0, pltpu.roll(r1, tok, 1))
        rks[1, :, 0:rows] = jnp.where(left, pltpu.roll(r0, tok, 1), r1)
        if r2 is not None:
            rks[0, :, rows : 2 * rows] = r2
            rks[1, :, rows : 2 * rows] = pltpu.roll(r2, tok, 1)

    lane = lax.broadcasted_iota(jnp.int32, (tok, HEAD_DIM), 1)

    def attend(c, js, lo, hi, nk, whole):
        row = lax.broadcasted_iota(jnp.int32, (tok, nk * tok), 0)
        col = lax.broadcasted_iota(jnp.int32, (tok, nk * tok), 1)
        allowed = (col <= row) | (col >= tok)
        units = [(j, h, slice(h * HEAD_DIM, (h + 1) * HEAD_DIM)) for j in js for h in range(2)]
        spans = range(lo, hi)
        scores = [
            lax.dot_general(
                qk[1, c, j, lo * tok : hi * tok, hs], qk[0, c, j, 0 : nk * tok, hs],
                (((1,), (1,)), ((), ())), preferred_element_type=F32,
            )
            for j, h, hs in units
        ]
        scaled = []
        for (j, h, hs), score in zip(units, scores):
            for s in spans:
                sc = score[(s - lo) * tok : (s - lo + 1) * tok]
                sc = sc * rqs[s, j * tok : (j + 1) * tok, 0 : nk * tok] * rks[j, 0:1, 0 : nk * tok]
                scaled.append(jnp.where(allowed, sc, -1e30) if s == 0 else sc)
        tops = [jnp.max(sc, axis=1, keepdims=True) for sc in scaled]
        expos = [jnp.exp(sc - top) for sc, top in zip(scaled, tops)]
        tots = [jnp.sum(e, axis=1, keepdims=True) for e in expos]
        n = hi - lo
        accs = []
        for i, (j, h, hs) in enumerate(units):
            w = [e.astype(BF16) for e in expos[i * n : (i + 1) * n]]
            w = w[0] if n == 1 else jnp.concatenate(w, axis=0)
            accs.append(jnp.dot(w, vbuf[c, j, 0 : nk * tok, hs], preferred_element_type=F32))
        for i, (j, h, hs) in enumerate(units):
            for s in spans:
                o = accs[i][(s - lo) * tok : (s - lo + 1) * tok] / tots[i * n + s - lo]
                if s == 0 and whole:
                    mixed[j * tok : (j + 1) * tok, pl.ds(pl.multiple_of(c * COLS + h * HEAD_DIM, HEAD_DIM), HEAD_DIM)] = o.astype(BF16)
                elif s == 0:
                    own_o[c, j, :, hs] = o
                else:
                    oout[s - 1, c, j, :, hs] = o.astype(BF16)
        for i, j in enumerate(js):
            for s in spans:
                if s == 0 and whole:
                    continue
                a, b = (tops[u] + jnp.log(tots[u]) for u in (2 * i * n + s - lo, (2 * i + 1) * n + s - lo))
                if s > 0:
                    lse_out[j, s - 1] = jnp.where(lane == 2 * c, a, jnp.where(lane == 2 * c + 1, b, lse_out[j, s - 1]))
                else:
                    own_lse[j] = jnp.where(lane == 2 * c, a, jnp.where(lane == 2 * c + 1, b, own_lse[j]))

    def remote_wait(c, j):
        with scope("attwait"):
            settle(blocks(2), q_recv.at[j, c])
            settle(blocks(2), kv_recv.at[j, c])

    def remote_part(c, j):
        remote_wait(c, j)
        attend(c, (j,), 1, 3, 2, False)
        o_copy(c, j, 2, 3).start()
        o_copy(c, j, 1, 2).start()

    def lifted_part(c, j):
        with scope("liftwait"):
            settle(blocks(1), q_recv.at[j, c])
            settle(blocks(4), kv_recv.at[j, c])
        attend(c, (j,), 0, 2, 3, True)
        o_copy(c, j, 1, 3).start()

    def send_lse(j):
        def message(a, b):
            lse_msg[j] = jnp.transpose(jnp.concatenate([a, b], axis=0))[0:16]

        @pl.when(z == 1)
        def _():
            message(lse_out[j, 0], lse_out[j, 1])
            l_copy(j, 2, 3).start()
            l_copy(j, 1, 2).start()

        @pl.when(z == 2)
        def _():
            message(lse_out[j, 0], lse_out[j, 0])
            l_copy(j, 1, 3).start()

    with scope("g2"):
        @pl.loop(0, nc)
        def _(c):
            acc = product(2 * nc + c)

            @pl.when(z == 0)
            def _():
                finish(acc, 1, c)

            @pl.when(z > 0)
            def _():
                keep_value(acc, c)

            @pl.when((z == 0) & (c >= LIFT[1]))
            def _():
                k_copy(c, 1, 1, 1).start()
                v_copy(c, 1, 1, 1).start()

            for j in range(2):

                @pl.when((z == 1) & (c < LIFT[j]))
                def _():
                    v_copy(c, j, 2, 2).start()

            @pl.when((z == 2) & (c >= LIFT[0]))
            def _():
                v_copy(c, 0, 1, 3).start()

            @pl.when((z == 2) & (c >= LIFT[1]))
            def _():
                q_copy(c, 1, 1, 1).start()

            @pl.when((z == 3) & (c >= LIFT[1]))
            def _():
                q_copy(c, 1, 2, 1).start()
                q_copy(c, 1, 1, 2).start()

            @pl.when((c == LIFT[0]) & (z == 1))
            def _():
                with scope("sw_near"):
                    a = near_scale(0)
                with scope("sw_far0"):
                    set_rk(a, far_scale(0))
                with scope("sw_far1"):
                    set_rq(1, far_scale(1))
                remote_wait(c, 0)
                attend(c, (0,), 1, 2, 2, False)
                o_copy(c, 0, 1, 2).start()
                with scope("sw_far2"):
                    set_rq(2, far_scale(2))
                attend(c, (0,), 2, 3, 2, False)
                o_copy(c, 0, 2, 3).start()

            @pl.when((z == 1) & (c > LIFT[0]))
            def _():
                remote_part(c, 0)

    @pl.when(z == 0)
    def _():
        @pl.loop(0, LIFT[1])
        def _(c):
            k_copy(c, 1, 1, 1).start()
            v_copy(c, 1, 1, 1).start()

        send_sums(1, 1)

    @pl.when(z == 1)
    def _():
        send_lse(0)

    @pl.when(z == 2)
    def _():
        with scope("sw_near"):
            set_rq(0, near_scale(0))
            r = near_scale(1)
            set_rk(r, r)
        with scope("own"):
            @pl.loop(LIFT[0], nc)
            def _(c):
                attend(c, (0,), 0, 1, 1, False)

        with scope("sw_far"):
            set_rk(r, far_scale(0), far_scale(1))
            set_rq(1, far_scale(2))
        with scope("lift"):
            for j in range(2):
                if j == 1:

                    @pl.loop(LIFT[1], nc)
                    def _(c):
                        settle(blocks(1), q_recv.at[1, c])
                        attend(c, (1,), 0, 2, 1, False)
                        o_copy(c, 1, 1, 3).start()

                @pl.loop(0, LIFT[j])
                def _(c):
                    lifted_part(c, j)

                send_lse(j)

    @pl.when(z == 0)
    def _():
        with scope("own"):
            r = near_scale(0)
            set_rk(r, r)
            set_rq(0, near_scale(1))

            @pl.loop(0, nc)
            def _(c):
                attend(c, (0, 1), 0, 1, 1, True)

    def merge(j, ni):
        lses = [own_lse[j]]
        settle(lse_in.at[pl.ds(0, ni), j], l_recv.at[j])
        for s in range(1, ni + 1):
            wide = jnp.concatenate([lse_in[s - 1, j], jnp.zeros((rows - 16, rows), F32)], axis=0)
            lses.append(jnp.transpose(wide)[(ni - 1) * tok : ni * tok])
        top = functools.reduce(jnp.maximum, lses)
        parts = [jnp.exp(v - top) for v in lses]
        tot = functools.reduce(jnp.add, parts)
        for s in range(ni + 1):
            shares[s] = parts[s] / tot

        def blend(c, slots):
            settle(blocks(len(slots)), o_recv.at[j, c])
            for h in range(2):
                hs = slice(h * HEAD_DIM, (h + 1) * HEAD_DIM)
                o = 0.0
                for s in (0, *slots):
                    share = jnp.sum(jnp.where(lane == 2 * c + h, shares[s], 0.0), axis=1, keepdims=True)
                    o += share * (own_o[c, j, :, hs] if s == 0 else oin[s - 1, c, j, :, hs].astype(F32))
                mixed[j * tok : (j + 1) * tok, pl.ds(pl.multiple_of(c * COLS + h * HEAD_DIM, HEAD_DIM), HEAD_DIM)] = o.astype(BF16)

        if ni == 2:

            @pl.loop(0, LIFT[j])
            def _(c):
                blend(c, (1,))

        @pl.loop(LIFT[j], nc)
        def _(c):
            blend(c, (1,) if ni == 1 else (2,) if j == 0 else (1, 2))

    share = tok // nt
    hc = oc // 2
    my, mx = me // 2, lax.rem(me, 2)

    def stage_one(n, j, half):
        if half == 0:
            src, to = part.at[n, j, half, :, 1 - mx], 2 * my + 1 - mx
        else:
            src, to = part.at[n, j, half, 1 - my], 2 * (1 - my) + mx
        return remote(src, rs_one.at[n, j, half], one_send, one_recv.at[j, n], (dp, z, to))

    def stage_two(n, j, half):
        to = 2 * (1 - my) + mx if half == 0 else 2 * my + 1 - mx
        return remote(rs_mid.at[n, j, half], rs_two.at[n, j, half], two_send, two_recv.at[j, n], (dp, z, to))

    def project_part(n, js, first_pass):
        lo, hi = js[0] * tok, (js[-1] + 1) * tok
        if first_pass:
            wo_copy(n).wait()
        acc = jnp.dot(mixed[lo:hi], wov[n], preferred_element_type=F32).astype(BF16)
        for j in js:
            for half in range(2):
                for t in range(nt):
                    row = j * tok + t * share - lo
                    part[n, j, half, t // 2, t % 2] = acc[row : row + share, half * hc : (half + 1) * hc]
                stage_one(n, j, half).start()

    def project(js, first_pass):
        @pl.loop(0, no)
        def _(n):
            project_part(n, js, first_pass)

    def forward(j):
        with scope("fwd"):
            @pl.loop(0, no)
            def _(n):
                settle(rs_one.at[n, j], one_recv.at[j, n])
                for half in range(2):
                    if half == 0:
                        o = part[n, j, half, 1 - my, mx].astype(F32) + rs_one[n, j, half, 1 - my].astype(F32)
                    else:
                        o = part[n, j, half, my, 1 - mx].astype(F32) + rs_one[n, j, half, 1 - mx].astype(F32)
                    rs_mid[n, j, half] = o.astype(BF16)
                    stage_two(n, j, half).start()

    def collect(j):
        with scope("collect"):
            @pl.loop(0, no)
            def _(n):
                settle(rs_two.at[n, j], two_recv.at[j, n])
                for half in range(2):
                    o = part[n, j, half, my, mx].astype(F32) + rs_one[n, j, half, my if half == 0 else mx].astype(F32)
                    o = o + rs_two[n, j, half].astype(F32)
                    out_ref[:, j, pl.ds(pl.multiple_of(n * oc + half * hc, hc), hc)] = o.astype(BF16)

    @pl.when(z == 0)
    def _():
        with scope("outp"):
            project((0, 1), True)

    @pl.when(z == 1)
    def _():
        def own(c, j):
            @pl.when(c < LIFT[j])
            def _():
                with scope("ownwait"):
                    settle(blocks(2), kv_recv.at[j, c])

            attend(c, (j,), 0, 1, 2, True)

        with scope("own0"):
            set_rq(0, near_scale(1))

            @pl.loop(0, nc)
            def _(i):
                own(lax.rem(i + LIFT[0], nc), 0)

        with scope("rem1"):
            @pl.loop(0, max(nc, no))
            def _(i):
                @pl.when((i >= LIFT[1]) & (i < nc))
                def _():
                    remote_part(i, 1)

                @pl.when(i < no)
                def _():
                    project_part(i, (0,), True)

            send_lse(1)

        with scope("own1"):
            @pl.loop(0, nc)
            def _(i):
                own(lax.rem(i + LIFT[1], nc), 1)

        with scope("outp"):
            project((1,), False)

    @pl.when(high)
    def _():
        for j in range(2):
            @pl.when(z == 2)
            def _():
                with scope("merge"):
                    merge(j, 1)

            @pl.when(z == 3)
            def _():
                if j == 0:
                    with scope("scales"):
                        set_rq(0, near_scale(0))
                        set_rk(near_scale(1), far_scale(0))
                with scope("own"):
                    alone = LIFT[0] if j == 0 else nc

                    @pl.loop(0, alone)
                    def _(c):
                        attend(c, (j,), 0, 1, 1, False)

                    if alone < nc:

                        @pl.loop(alone, nc)
                        def _(c):
                            with scope("ownwait"):
                                settle(blocks(2), kv_recv.at[j, c])
                            attend(c, (j,), 0, 1, 2, False)

                with scope("merge"):
                    merge(j, 2)

            with scope("outp"):
                project((j,), j == 0)

    for j in range(2):
        forward(j)
    for j in range(2):
        collect(j)

    _t = scope("tail")
    _t.__enter__()
    settle(rs_one, one_send)
    settle(rs_mid, two_send)
    for g in range(2):
        settle(sums_in.at[g], sum_send.at[g])

    up = sum(LIFT)
    down = 2 * nc - up

    @pl.when(z == 0)
    def _():
        for i, count in enumerate((2 * nc, up)):
            settle(sums_far.at[0], far_send.at[i])
            settle(blocks(count), k_send.at[i])
            settle(blocks(count), v_send.at[i])

    @pl.when(z == 1)
    def _():
        settle(sums_far.at[0], far_send.at[0])
        settle(blocks(up), k_send.at[1])
        settle(blocks(up), v_send.at[1])
        for i in range(2):
            settle(lse_msg, l_send.at[i])
            settle(blocks(down), o_send.at[i])

    @pl.when(z == 2)
    def _():
        for i in range(2):
            settle(sums_far.at[0], far_send.at[i])
        settle(lse_msg, l_send.at[0])
        settle(blocks(LIFT[0] + nc), o_send.at[0])
        settle(blocks(down), q_send.at[0])
        settle(blocks(nc - LIFT[0]), k_send.at[2])
        settle(blocks(nc - LIFT[0]), v_send.at[2])

    @pl.when(z == 3)
    def _():
        for i, count in enumerate((LIFT[0] + nc, down)):
            settle(sums_far.at[0], far_send.at[i])
            settle(blocks(count), q_send.at[i])

    _t.__exit__(None, None, None)


def fused(ns, nt, tokens, w_query, w_key, w_value, w_out, gain_query, gain_key):
    tok, seqs, depth = tokens.shape
    local = w_query.shape[1]
    nc = local // COLS
    oc = 1024
    no = depth // oc
    rows = tok * seqs
    width = HEADS * HEAD_DIM
    vm = pltpu.VMEM
    dma = pltpu.SemaphoreType.DMA
    scratch = [
        vm((local,), F32), vm((local,), F32),
        vm((RING, depth, COLS), BF16), vm((no, local, oc), BF16),
        vm((tok, seqs, depth), BF16), vm((rows, depth), BF16), vm((rows, depth), BF16),
        vm((rows, HEAD_DIM), F32), vm((rows, HEAD_DIM), F32), vm((2, nc, 1, COLS), F32), vm((2, rows, HEAD_DIM), F32),
        vm((2, 8, rows), F32), vm((2, nt - 1, 8, rows), F32), vm((3, nt, 8, rows), F32),
        vm((3, rows, 2 * rows), F32), vm((2, 8, 2 * rows), F32),
        vm((2, nc, seqs, 3 * tok, COLS), BF16), vm((nc, seqs, 3 * tok, COLS), BF16),
        vm((nc, seqs, tok, COLS), F32), vm((seqs, tok, HEAD_DIM), F32),
        vm((2, nc, seqs, tok, COLS), BF16), vm((seqs, 2, tok, HEAD_DIM), F32), vm((seqs, 16, rows), F32),
        vm((2, nc, seqs, tok, COLS), BF16), vm((2, seqs, 16, rows), F32), vm((3, tok, HEAD_DIM), F32),
        vm((rows, local), BF16), vm((no, seqs, 2, 2, 2, tok // nt, oc // 2), BF16),
        vm((no, seqs, 2, 2, tok // nt, oc // 2), BF16), vm((no, seqs, 2, tok // nt, oc // 2), BF16), vm((no, seqs, 2, tok // nt, oc // 2), BF16),
        dma, dma((2,)), dma((RING,)), dma((no,)), dma((2,)), dma((2,)), dma((2,)), dma((3,)), dma((3,)), dma((3,)), dma((2, nc)),
        dma((2,)), dma((2, nc)), dma((2,)), dma((2, nc)), dma((2,)), dma((2,)), dma, dma((2, no)), dma, dma((2, no)),
    ]
    in_vmem = pl.BlockSpec(memory_space=pltpu.VMEM)
    in_hbm = pl.BlockSpec(memory_space=pltpu.HBM)
    return pl.pallas_call(
        functools.partial(block_kernel, ns, nt, tok, width),
        out_shape=pltpu.VMEM((tok // nt, seqs, depth), BF16),
        in_specs=[in_hbm] * 7,
        out_specs=in_vmem,
        scratch_shapes=scratch,
        compiler_params=pltpu.CompilerParams(collective_id=0, has_side_effects=True, vmem_limit_bytes=58 * 1024 * 1024),
    )(tokens, gain_query, gain_key, w_query, w_key, w_value, w_out)


def rotary(field, positions):
    half = HEAD_DIM // 2
    shaped = field.reshape(field.shape[0], -1, HEAD_DIM)
    freqs = jnp.exp(-jnp.log(500000.0) * jnp.arange(half, dtype=jnp.float32) * 2.0 / HEAD_DIM)
    angle = positions.astype(jnp.float32)[:, None] * freqs[None, :]
    cosine = jnp.cos(angle)[:, None, :]
    sine = jnp.sin(angle)[:, None, :]
    first = shaped[..., :half]
    second = shaped[..., half:]
    turned = jnp.concatenate(
        [first * cosine - second * sine, second * cosine + first * sine], axis=-1
    )
    return turned.reshape(field.shape[0], -1)


def local(tokens, w_query, w_key, w_value, w_out, gain_query, gain_key):
    tok_rows = tokens.shape[0]
    seq_count = tokens.shape[1]
    local_width = w_query.shape[1]
    local_heads = local_width // HEAD_DIM
    width = HEADS * HEAD_DIM
    flat = tokens.reshape(tok_rows * seq_count, tokens.shape[2])
    query = jnp.dot(flat, w_query, preferred_element_type=jnp.float32)
    key_raw = jnp.dot(flat, w_key, preferred_element_type=jnp.float32)
    sum_query, sum_key = lax.psum(
        (jnp.sum(query * query, axis=1), jnp.sum(key_raw * key_raw, axis=1)), "tensor"
    )
    value = jnp.dot(flat, w_value, preferred_element_type=jnp.float32).astype(jnp.bfloat16)
    scale_q = lax.rsqrt(sum_query / width + 1e-06)
    scale_k = lax.rsqrt(sum_key / width + 1e-06)
    my_block = lax.axis_index("seq")
    positions = my_block * tok_rows + jnp.arange(tok_rows, dtype=jnp.int32)
    row_positions = (positions[:, None] + jnp.zeros((1, seq_count), jnp.int32)).reshape(-1)
    q_normed = rotary(query * scale_q[:, None] * gain_query[None, :], row_positions).astype(
        jnp.bfloat16
    )
    k_normed = rotary(key_raw * scale_k[:, None] * gain_key[None, :], row_positions).astype(
        jnp.bfloat16
    )
    q_heads = q_normed.reshape(tok_rows, seq_count, local_heads, HEAD_DIM)
    k_local = k_normed.reshape(tok_rows, seq_count, local_width)
    v_local = value.reshape(tok_rows, seq_count, local_width)
    factor = HEAD_DIM ** (-0.5)
    piece = (
        lax.all_gather(k_local, "seq", axis=0, tiled=True),
        lax.all_gather(v_local, "seq", axis=0, tiled=True),
    )
    key_pos = jnp.arange(piece[0].shape[0], dtype=jnp.int32)
    key_block = piece[0]
    count = key_block.shape[0]
    key_heads = key_block.reshape(count, seq_count, local_heads, HEAD_DIM)
    value_heads = piece[1].reshape(count, seq_count, local_heads, HEAD_DIM)
    scores = (
        jnp.einsum("qshd,kshd->shqk", q_heads, key_heads, preferred_element_type=jnp.float32)
        * factor
    )
    allowed = (key_pos[None, None, None, :] <= positions[None, None, :, None]) & (
        key_pos[None, None, None, :] >= 0
    )
    old_max = jnp.full((seq_count, local_heads, tok_rows), -1e30, jnp.float32)
    new_max = jnp.maximum(old_max, jnp.max(jnp.where(allowed, scores, -1e30), axis=3))
    expo = jnp.where(allowed, jnp.exp(scores - new_max[..., None]), 0.0)
    new_total = jnp.sum(expo, axis=3)
    added = jnp.einsum(
        "shqk,kshd->shqd",
        expo.astype(jnp.bfloat16),
        value_heads,
        preferred_element_type=jnp.float32,
    )
    final_state = (new_max, new_total, added)
    final_max, final_total, final_acc = final_state
    mixed = (final_acc / final_total[..., None]).astype(jnp.bfloat16)
    mixed = jnp.transpose(mixed, (2, 0, 1, 3)).reshape(tok_rows, seq_count, local_width)
    return lax.psum_scatter(
        jnp.dot(mixed, w_out, preferred_element_type=jnp.float32).astype(jnp.bfloat16),
        "tensor",
        scatter_dimension=0,
        tiled=True,
    )


def solution(mesh):
    ns, nt = mesh.shape["seq"], mesh.shape["tensor"]
    step = functools.partial(fused, ns, nt) if ns == 4 and nt == 4 else local
    return jax.shard_map(
        step,
        mesh=mesh,
        in_specs=(
            P("seq", "dp", None),
            P(None, "tensor"),
            P(None, "tensor"),
            P(None, "tensor"),
            P("tensor", None),
            P("tensor"),
            P("tensor"),
        ),
        out_specs=P(("seq", "tensor"), "dp", None),
        check_vma=False,
    )
```

```python
import contextlib
import functools

import jax
import jax.numpy as jnp
from jax import lax
from jax.experimental import pallas as pl
from jax.experimental.pallas import tpu as pltpu
from jax.sharding import PartitionSpec as P

HEADS = 40
HEAD_DIM = 128
MESH = pl.DeviceIdType.MESH
COLS = 2 * HEAD_DIM
RING = 9
LIFT = (1, 1)
F32 = jnp.float32
BF16 = jnp.bfloat16


def scope(name):
    return contextlib.nullcontext()


def block_kernel(
    ns, nt, tok, width,
    x_hbm, gq_hbm, gk_hbm, wq, wk, wv, wo,
    out_ref,
    gq_in, gk_in, ring, wov, xin, xi, xs, cos_ref, sin_ref, gains, ssq,
    sums_out, sums_in, sums_far, rqs, rks,
    qk, vbuf, own_o, own_lse, oout, lse_out, lse_msg, oin, lse_in, shares,
    mixed, part, rs_one, rs_mid, rs_two,
    x_sem, g_sem, w_sem, wo_sem, sum_send, sum_recv, far_send, far_recv, k_send, v_send, kv_recv,
    q_send, q_recv, o_send, o_recv, l_send, l_recv, one_send, one_recv, two_send, two_recv,
):
    dp = lax.axis_index("dp")
    z = lax.axis_index("seq")
    me = lax.axis_index("tensor")
    low = z < 2
    high = z >= 2
    nc = vbuf.shape[0]
    rows = 2 * tok
    oc = wov.shape[2]
    no = wov.shape[0]

    def w_copy(ref, c, slot):
        return pltpu.make_async_copy(
            ref.at[:, pl.ds(pl.multiple_of(c * COLS, COLS), COLS)], ring.at[slot], w_sem.at[slot]
        )

    def wo_copy(c):
        return pltpu.make_async_copy(
            wo.at[:, pl.ds(pl.multiple_of(c * oc, oc), oc)], wov.at[c], wo_sem.at[c]
        )

    def start(i):
        slot = lax.rem(i, RING)
        group = i // nc
        c = i - group * nc
        inside = i < 3 * nc

        @pl.when(inside & ((low & (group == 0)) | (high & (group == 1))))
        def _():
            w_copy(wk, c, slot).start()

        @pl.when(inside & (((z == 0) & (group == 1)) | ((z > 0) & (group == 2))))
        def _():
            w_copy(wv, c, slot).start()

        @pl.when(inside & (((z == 0) & (group == 2)) | ((z == 1) & (group == 1)) | (high & (group == 0))))
        def _():
            w_copy(wq, c, slot).start()

        @pl.when((i >= 3 * nc) & (i < 3 * nc + no))
        def _():
            wo_copy(i - 3 * nc).start()

    x_copy = pltpu.make_async_copy(x_hbm, xin, x_sem)
    x_copy.start()
    g_copies = [pltpu.make_async_copy(gk_hbm, gk_in, g_sem.at[0]), pltpu.make_async_copy(gq_hbm, gq_in, g_sem.at[1])]
    for copy in g_copies:
        copy.start()

    barrier = pltpu.get_barrier_semaphore()
    linked = {0: (1, 2), 1: (0, 2, 3), 2: (0, 1, 3), 3: (1, 2)}
    for d in range(1, nt):
        pl.semaphore_signal(barrier, inc=1, device_id=(dp, z, lax.rem(me + d, nt)), device_id_type=MESH)
    for a in range(ns):
        hit = functools.reduce(jnp.logical_or, [z == b for b in linked[a]])

        @pl.when(hit)
        def _():
            for d in range(nt):
                pl.semaphore_signal(barrier, inc=1, device_id=(dp, a, lax.rem(me + d, nt)), device_id_type=MESH)

    def greet():
        pl.semaphore_wait(barrier, nt - 1 + nt * jnp.where((z == 1) | (z == 2), 3, 2))

    def remote(src, dst, ssem, rsem, to):
        return pltpu.make_async_remote_copy(
            src_ref=src, dst_ref=dst, send_sem=ssem, recv_sem=rsem, device_id=to, device_id_type=MESH
        )

    def settle(ref, sem):
        pltpu.make_async_copy(ref, ref, sem).wait()

    def blocks(count):
        return xi.at[:, pl.ds(0, count * HEAD_DIM)]

    def k_copy(c, j, b, to):
        at = b * tok
        return remote(qk.at[0, c, j, pl.ds(0, tok)], qk.at[0, c, j, pl.ds(at, tok)], k_send.at[to - 1], kv_recv.at[j, c], (dp, to, me))

    def v_copy(c, j, b, to):
        at = b * tok
        return remote(vbuf.at[c, j, pl.ds(0, tok)], vbuf.at[c, j, pl.ds(at, tok)], v_send.at[to - 1], kv_recv.at[j, c], (dp, to, me))

    def q_copy(c, j, s, to):
        return remote(qk.at[1, c, j, pl.ds(0, tok)], qk.at[1, c, j, pl.ds(s * tok, tok)], q_send.at[s - 1], q_recv.at[j, c], (dp, to, me))

    def o_copy(c, j, s, to):
        return remote(oout.at[s - 1, c, j], oin.at[s - 1, c, j], o_send.at[s - 1], o_recv.at[j, c], (dp, to, me))

    def l_copy(j, s, to):
        return remote(lse_msg.at[j], lse_in.at[s - 1, j], l_send.at[s - 1], l_recv.at[j], (dp, to, me))

    def near(g, d):
        return remote(sums_out.at[g], sums_in.at[g, d - 1], sum_send.at[g], sum_recv.at[g], (dp, z, lax.rem(me + d, nt)))

    def far(d, slot, ss, to, g=0):
        return remote(sums_out.at[g], sums_far.at[slot, d], far_send.at[ss], far_recv.at[slot], (dp, to, lax.rem(me + d, nt)))

    def product(i):
        slot = lax.rem(i, RING)
        start(i + RING - 1)
        with scope("wwait"):
            w_copy(wk, 0, slot).wait()
        return jnp.dot(xs[...], ring[slot], preferred_element_type=F32)

    def turned(acc, kind, c):
        cosine, sine = cos_ref[...], sin_ref[...]
        for h in range(2):
            y = acc[:, h * HEAD_DIM : (h + 1) * HEAD_DIM] * gains[kind, c, :, h * HEAD_DIM : (h + 1) * HEAD_DIM]
            y = (y * cosine + pltpu.roll(y, HEAD_DIM // 2, 1) * sine).astype(BF16)
            for j in range(2):
                qk[kind, c, j, 0:tok, h * HEAD_DIM : (h + 1) * HEAD_DIM] = y[j * tok : (j + 1) * tok]

    def finish(acc, kind, c):
        ssq[kind] += acc[:, :HEAD_DIM] * acc[:, :HEAD_DIM] + acc[:, HEAD_DIM:] * acc[:, HEAD_DIM:]
        turned(acc, kind, c)

    def keep_value(acc, c):
        v = acc.astype(BF16)
        for j in range(2):
            vbuf[c, j, 0:tok, :] = v[j * tok : (j + 1) * tok]

    with scope("init"):
        lanes = lax.broadcasted_iota(jnp.int32, (tok, HEAD_DIM), 1)
        half = HEAD_DIM // 2
        freqs = jnp.exp(-jnp.log(500000.0) * lax.rem(lanes, half).astype(F32) * 2.0 / HEAD_DIM)
        spot = z * tok + lax.broadcasted_iota(jnp.int32, (tok, HEAD_DIM), 0)
        angle = spot.astype(F32) * freqs
        cosine = jnp.cos(angle)
        sine = jnp.sin(angle)
        sine = jnp.where(lanes < half, -sine, sine)
        for j in range(2):
            cos_ref[j * tok : (j + 1) * tok] = cosine
            sin_ref[j * tok : (j + 1) * tok] = sine

        @pl.loop(0, RING - 1)
        def _(i):
            start(i)

        for copy in g_copies:
            copy.wait()
        for c in range(nc):
            gains[0, c] = gk_in[c * COLS : (c + 1) * COLS].reshape(1, COLS)
            gains[1, c] = gq_in[c * COLS : (c + 1) * COLS].reshape(1, COLS)
        ssq[...] = jnp.zeros_like(ssq)
        sums_out[...] = jnp.zeros_like(sums_out)
        own_lse[...] = jnp.zeros_like(own_lse)
        lse_out[...] = jnp.full_like(lse_out, -1e30)

    with scope("xwait"):
        x_copy.wait()
    with scope("xlay"):
        @pl.loop(0, tok // 8)
        def _(i):
            v = xin[pl.ds(pl.multiple_of(i * 8, 8), 8)]
            xi[pl.ds(pl.multiple_of(i * 16, 16), 16), :] = v.reshape(16, v.shape[-1])

        r = lax.broadcasted_iota(jnp.int32, (rows, rows), 0)
        q = lax.broadcasted_iota(jnp.int32, (rows, rows), 1)
        pick = (q == jnp.where(r < tok, 2 * r, 2 * (r - tok) + 1)).astype(F32).astype(BF16)

        half_depth = xs.shape[1] // 2
        for i in range(2):
            at = slice(i * half_depth, (i + 1) * half_depth)
            xs[:, at] = jnp.dot(pick, xi[:, at], preferred_element_type=F32).astype(BF16)

    def fill_sums(g, kind):
        sums_out[g, 0:1, :] = jnp.sum(jnp.transpose(ssq[kind]), axis=0, keepdims=True)

    def send_near(g):
        for d in range(1, nt):
            near(g, d).start()

    def send_sums(g, kind):
        fill_sums(g, kind)
        send_near(g)

    first = jnp.where(low, 0, 1)
    second = jnp.where(z == 1, 1, 0)

    with scope("g0"):
        @pl.loop(0, nc)
        def _(c):
            acc = product(c)

            @pl.when((c == 0) & ((z == 0) | (z == 3)))
            def _():
                greet()

            finish(acc, first, c)

            @pl.when((z == 0) & (c < LIFT[0]))
            def _():
                k_copy(c, 0, 1, 2).start()

            @pl.when((z == 0) & (c >= LIFT[0]))
            def _():
                k_copy(c, 0, 1, 1).start()

            @pl.when((z == 3) & (c < LIFT[0]))
            def _():
                q_copy(c, 0, 1, 2).start()

            @pl.when((z == 3) & (c >= LIFT[0]) & (c < nc - 2))
            def _():
                q_copy(c, 0, 2, 1).start()

    @pl.when((z == 1) | (z == 2))
    def _():
        with scope("barwait"):
            greet()

    fill_sums(0, first)

    @pl.when(z == 0)
    def _():
        for to in (1, 2):
            for d in range(nt):
                far(d, 0, to - 1, to).start()

    @pl.when(z == 1)
    def _():
        for d in range(nt):
            far(d, 1, 0, 2).start()

    @pl.when(z == 2)
    def _():
        for d in range(nt):
            far(d, 1, 0, 1).start()

    @pl.when(z == 3)
    def _():
        for to in (1, 2):
            for d in range(nt):
                far(d, 2, to - 1, to).start()

    send_near(0)

    @pl.when(z == 3)
    def _():
        @pl.loop(nc - 2, nc)
        def _(c):
            q_copy(c, 0, 2, 1).start()

    @pl.when(z == 1)
    def _():
        for j in range(2):

            @pl.loop(0, LIFT[j])
            def _(c):
                k_copy(c, j, 2, 2).start()

    with scope("g1"):
        @pl.loop(0, nc)
        def _(c):
            acc = product(nc + c)

            @pl.when(z == 0)
            def _():
                keep_value(acc, c)

            @pl.when(z > 0)
            def _():
                finish(acc, second, c)

            @pl.when((z == 0) & (c < LIFT[0]))
            def _():
                v_copy(c, 0, 1, 2).start()

            @pl.when((z == 0) & (c >= LIFT[0]))
            def _():
                v_copy(c, 0, 1, 1).start()

            @pl.when((z == 2) & (c >= LIFT[0]))
            def _():
                q_copy(c, 0, 1, 1).start()
                k_copy(c, 0, 1, 3).start()

            @pl.when((z == 3) & (c < LIFT[1]))
            def _():
                q_copy(c, 1, 1, 2).start()

    @pl.when(z > 0)
    def _():
        fill_sums(1, second)

        @pl.when(z == 2)
        def _():
            for d in range(nt):
                far(d, 0, 1, 3, 1).start()

        send_near(1)

    @pl.when(z == 0)
    def _():
        for j, to in ((1, 2), (0, 1)):

            @pl.loop(0, LIFT[j])
            def _(c):
                k_copy(c, j, 1, to).start()
                v_copy(c, j, 1, to).start()

    def near_scale(g):
        settle(sums_in.at[g], sum_recv.at[g])
        tot = sums_out[g]
        for d in range(1, nt):
            tot = tot + sums_in[g, d - 1]
        return lax.rsqrt(tot / width + 1e-06)

    def far_scale(slot):
        settle(sums_far.at[slot], far_recv.at[slot])
        tot = sums_far[slot, 0]
        for d in range(1, nt):
            tot = tot + sums_far[slot, d]
        return lax.rsqrt(tot / width + 1e-06)

    def set_rq(s, r):
        rqs[s] = jnp.transpose(jnp.broadcast_to(r[0:1, :] * HEAD_DIM ** (-0.5), (2 * rows, rows)))

    def set_rk(r0, r1, r2=None):
        left = lax.broadcasted_iota(jnp.int32, r0.shape, 1) < tok
        rks[0, :, 0:rows] = jnp.where(left, r0, pltpu.roll(r1, tok, 1))
        rks[1, :, 0:rows] = jnp.where(left, pltpu.roll(r0, tok, 1), r1)
        if r2 is not None:
            rks[0, :, rows : 2 * rows] = r2
            rks[1, :, rows : 2 * rows] = pltpu.roll(r2, tok, 1)

    lane = lax.broadcasted_iota(jnp.int32, (tok, HEAD_DIM), 1)

    def attend(c, js, lo, hi, nk, whole):
        row = lax.broadcasted_iota(jnp.int32, (tok, nk * tok), 0)
        col = lax.broadcasted_iota(jnp.int32, (tok, nk * tok), 1)
        allowed = (col <= row) | (col >= tok)
        units = [(j, h, slice(h * HEAD_DIM, (h + 1) * HEAD_DIM)) for j in js for h in range(2)]
        spans = range(lo, hi)
        scores = [
            lax.dot_general(
                qk[1, c, j, lo * tok : hi * tok, hs], qk[0, c, j, 0 : nk * tok, hs],
                (((1,), (1,)), ((), ())), preferred_element_type=F32,
            )
            for j, h, hs in units
        ]
        scaled = []
        for (j, h, hs), score in zip(units, scores):
            for s in spans:
                sc = score[(s - lo) * tok : (s - lo + 1) * tok]
                sc = sc * rqs[s, j * tok : (j + 1) * tok, 0 : nk * tok] * rks[j, 0:1, 0 : nk * tok]
                scaled.append(jnp.where(allowed, sc, -1e30) if s == 0 else sc)
        tops = [jnp.max(sc, axis=1, keepdims=True) for sc in scaled]
        expos = [jnp.exp(sc - top) for sc, top in zip(scaled, tops)]
        tots = [jnp.sum(e, axis=1, keepdims=True) for e in expos]
        n = hi - lo
        accs = []
        for i, (j, h, hs) in enumerate(units):
            w = [e.astype(BF16) for e in expos[i * n : (i + 1) * n]]
            w = w[0] if n == 1 else jnp.concatenate(w, axis=0)
            accs.append(jnp.dot(w, vbuf[c, j, 0 : nk * tok, hs], preferred_element_type=F32))
        for i, (j, h, hs) in enumerate(units):
            for s in spans:
                o = accs[i][(s - lo) * tok : (s - lo + 1) * tok] / tots[i * n + s - lo]
                if s == 0 and whole:
                    mixed[j * tok : (j + 1) * tok, pl.ds(pl.multiple_of(c * COLS + h * HEAD_DIM, HEAD_DIM), HEAD_DIM)] = o.astype(BF16)
                elif s == 0:
                    own_o[c, j, :, hs] = o
                else:
                    oout[s - 1, c, j, :, hs] = o.astype(BF16)
        for i, j in enumerate(js):
            for s in spans:
                if s == 0 and whole:
                    continue
                a, b = (tops[u] + jnp.log(tots[u]) for u in (2 * i * n + s - lo, (2 * i + 1) * n + s - lo))
                if s > 0:
                    lse_out[j, s - 1] = jnp.where(lane == 2 * c, a, jnp.where(lane == 2 * c + 1, b, lse_out[j, s - 1]))
                else:
                    own_lse[j] = jnp.where(lane == 2 * c, a, jnp.where(lane == 2 * c + 1, b, own_lse[j]))

    def remote_wait(c, j):
        with scope("attwait"):
            settle(blocks(2), q_recv.at[j, c])
            settle(blocks(2), kv_recv.at[j, c])

    def remote_part(c, j):
        remote_wait(c, j)
        attend(c, (j,), 1, 3, 2, False)
        o_copy(c, j, 2, 3).start()
        o_copy(c, j, 1, 2).start()

    def lifted_part(c, j):
        with scope("liftwait"):
            settle(blocks(1), q_recv.at[j, c])
            settle(blocks(4), kv_recv.at[j, c])
        attend(c, (j,), 0, 2, 3, True)
        o_copy(c, j, 1, 3).start()

    def send_lse(j):
        def message(a, b):
            lse_msg[j] = jnp.transpose(jnp.concatenate([a, b], axis=0))[0:16]

        @pl.when(z == 1)
        def _():
            message(lse_out[j, 0], lse_out[j, 1])
            l_copy(j, 2, 3).start()
            l_copy(j, 1, 2).start()

        @pl.when(z == 2)
        def _():
            message(lse_out[j, 0], lse_out[j, 0])
            l_copy(j, 1, 3).start()

    with scope("g2"):
        @pl.loop(0, nc)
        def _(c):
            acc = product(2 * nc + c)

            @pl.when(z == 0)
            def _():
                finish(acc, 1, c)

            @pl.when(z > 0)
            def _():
                keep_value(acc, c)

            @pl.when((z == 0) & (c >= LIFT[1]))
            def _():
                k_copy(c, 1, 1, 1).start()
                v_copy(c, 1, 1, 1).start()

            for j in range(2):

                @pl.when((z == 1) & (c < LIFT[j]))
                def _():
                    v_copy(c, j, 2, 2).start()

            @pl.when((z == 2) & (c >= LIFT[0]))
            def _():
                v_copy(c, 0, 1, 3).start()

            @pl.when((z == 2) & (c >= LIFT[1]))
            def _():
                q_copy(c, 1, 1, 1).start()

            @pl.when((z == 3) & (c >= LIFT[1]))
            def _():
                q_copy(c, 1, 2, 1).start()
                q_copy(c, 1, 1, 2).start()

            @pl.when((c == LIFT[0]) & (z == 1))
            def _():
                with scope("sw_near"):
                    a = near_scale(0)
                with scope("sw_far0"):
                    set_rk(a, far_scale(0))
                with scope("sw_far1"):
                    set_rq(1, far_scale(1))
                remote_wait(c, 0)
                attend(c, (0,), 1, 2, 2, False)
                o_copy(c, 0, 1, 2).start()
                with scope("sw_far2"):
                    set_rq(2, far_scale(2))
                attend(c, (0,), 2, 3, 2, False)
                o_copy(c, 0, 2, 3).start()

            @pl.when((z == 1) & (c > LIFT[0]))
            def _():
                remote_part(c, 0)

    @pl.when(z == 0)
    def _():
        @pl.loop(0, LIFT[1])
        def _(c):
            k_copy(c, 1, 1, 1).start()
            v_copy(c, 1, 1, 1).start()

        send_sums(1, 1)

    @pl.when(z == 1)
    def _():
        send_lse(0)

    @pl.when(z == 2)
    def _():
        with scope("sw_near"):
            set_rq(0, near_scale(0))
            r = near_scale(1)
            set_rk(r, r)
        with scope("own"):
            @pl.loop(LIFT[0], nc)
            def _(c):
                attend(c, (0,), 0, 1, 1, False)

        with scope("sw_far"):
            set_rk(r, far_scale(0), far_scale(1))
            set_rq(1, far_scale(2))
        with scope("lift"):
            for j in range(2):
                if j == 1:

                    @pl.loop(LIFT[1], nc)
                    def _(c):
                        settle(blocks(1), q_recv.at[1, c])
                        attend(c, (1,), 0, 2, 1, False)
                        o_copy(c, 1, 1, 3).start()

                @pl.loop(0, LIFT[j])
                def _(c):
                    lifted_part(c, j)

                send_lse(j)

    @pl.when(z == 0)
    def _():
        with scope("own"):
            r = near_scale(0)
            set_rk(r, r)
            set_rq(0, near_scale(1))

            @pl.loop(0, nc)
            def _(c):
                attend(c, (0, 1), 0, 1, 1, True)

    def merge(j, ni):
        lses = [own_lse[j]]
        settle(lse_in.at[pl.ds(0, ni), j], l_recv.at[j])
        for s in range(1, ni + 1):
            wide = jnp.concatenate([lse_in[s - 1, j], jnp.zeros((rows - 16, rows), F32)], axis=0)
            lses.append(jnp.transpose(wide)[(ni - 1) * tok : ni * tok])
        top = functools.reduce(jnp.maximum, lses)
        parts = [jnp.exp(v - top) for v in lses]
        tot = functools.reduce(jnp.add, parts)
        for s in range(ni + 1):
            shares[s] = parts[s] / tot

        def blend(c, slots):
            settle(blocks(len(slots)), o_recv.at[j, c])
            for h in range(2):
                hs = slice(h * HEAD_DIM, (h + 1) * HEAD_DIM)
                o = 0.0
                for s in (0, *slots):
                    share = jnp.sum(jnp.where(lane == 2 * c + h, shares[s], 0.0), axis=1, keepdims=True)
                    o += share * (own_o[c, j, :, hs] if s == 0 else oin[s - 1, c, j, :, hs].astype(F32))
                mixed[j * tok : (j + 1) * tok, pl.ds(pl.multiple_of(c * COLS + h * HEAD_DIM, HEAD_DIM), HEAD_DIM)] = o.astype(BF16)

        if ni == 2:

            @pl.loop(0, LIFT[j])
            def _(c):
                blend(c, (1,))

        @pl.loop(LIFT[j], nc)
        def _(c):
            blend(c, (1,) if ni == 1 else (2,) if j == 0 else (1, 2))

    share = tok // nt
    hc = oc // 2
    my, mx = me // 2, lax.rem(me, 2)

    def stage_one(n, j, half):
        if half == 0:
            src, to = part.at[n, j, half, :, 1 - mx], 2 * my + 1 - mx
        else:
            src, to = part.at[n, j, half, 1 - my], 2 * (1 - my) + mx
        return remote(src, rs_one.at[n, j, half], one_send, one_recv.at[j, n], (dp, z, to))

    def stage_two(n, j, half):
        to = 2 * (1 - my) + mx if half == 0 else 2 * my + 1 - mx
        return remote(rs_mid.at[n, j, half], rs_two.at[n, j, half], two_send, two_recv.at[j, n], (dp, z, to))

    def project_part(n, js, first_pass):
        lo, hi = js[0] * tok, (js[-1] + 1) * tok
        if first_pass:
            wo_copy(n).wait()
        acc = jnp.dot(mixed[lo:hi], wov[n], preferred_element_type=F32).astype(BF16)
        for j in js:
            for half in range(2):
                for t in range(nt):
                    row = j * tok + t * share - lo
                    part[n, j, half, t // 2, t % 2] = acc[row : row + share, half * hc : (half + 1) * hc]
                stage_one(n, j, half).start()

    def project(js, first_pass):
        @pl.loop(0, no, unroll=not first_pass)
        def _(n):
            project_part(n, js, first_pass)

    def forward(j):
        with scope("fwd"):
            @pl.loop(0, no)
            def _(n):
                settle(rs_one.at[n, j], one_recv.at[j, n])
                for half in range(2):
                    if half == 0:
                        o = part[n, j, half, 1 - my, mx].astype(F32) + rs_one[n, j, half, 1 - my].astype(F32)
                    else:
                        o = part[n, j, half, my, 1 - mx].astype(F32) + rs_one[n, j, half, 1 - mx].astype(F32)
                    rs_mid[n, j, half] = o.astype(BF16)
                    stage_two(n, j, half).start()

    def collect(j):
        with scope("collect"):
            @pl.loop(0, no)
            def _(n):
                settle(rs_two.at[n, j], two_recv.at[j, n])
                for half in range(2):
                    o = part[n, j, half, my, mx].astype(F32) + rs_one[n, j, half, my if half == 0 else mx].astype(F32)
                    o = o + rs_two[n, j, half].astype(F32)
                    out_ref[:, j, pl.ds(pl.multiple_of(n * oc + half * hc, hc), hc)] = o.astype(BF16)

    @pl.when(z == 0)
    def _():
        with scope("outp"):
            project((0, 1), True)

    @pl.when(z == 1)
    def _():
        def own(c, j):
            @pl.when(c < LIFT[j])
            def _():
                with scope("ownwait"):
                    settle(blocks(2), kv_recv.at[j, c])

            attend(c, (j,), 0, 1, 2, True)

        with scope("own0"):
            set_rq(0, near_scale(1))

            @pl.loop(0, nc)
            def _(i):
                own(lax.rem(i + LIFT[0], nc), 0)

        with scope("rem1"):
            @pl.loop(0, max(nc, no))
            def _(i):
                @pl.when((i >= LIFT[1]) & (i < nc))
                def _():
                    remote_part(i, 1)

                @pl.when(i < no)
                def _():
                    project_part(i, (0,), True)

            send_lse(1)

        with scope("own1"):
            @pl.loop(0, nc)
            def _(i):
                own(lax.rem(i + LIFT[1], nc), 1)

        with scope("outp"):
            project((1,), False)

    @pl.when(high)
    def _():
        for j in range(2):
            @pl.when(z == 2)
            def _():
                with scope("merge"):
                    merge(j, 1)

            @pl.when(z == 3)
            def _():
                if j == 0:
                    with scope("scales"):
                        set_rq(0, near_scale(0))
                        set_rk(near_scale(1), far_scale(0))
                with scope("own"):
                    alone = LIFT[0] if j == 0 else nc

                    @pl.loop(0, alone)
                    def _(c):
                        attend(c, (j,), 0, 1, 1, False)

                    if alone < nc:

                        @pl.loop(alone, nc)
                        def _(c):
                            with scope("ownwait"):
                                settle(blocks(2), kv_recv.at[j, c])
                            attend(c, (j,), 0, 1, 2, False)

                with scope("merge"):
                    merge(j, 2)

            with scope("outp"):
                project((j,), j == 0)

    for j in range(2):
        forward(j)
    for j in range(2):
        collect(j)

    _t = scope("tail")
    _t.__enter__()
    settle(rs_one, one_send)
    settle(rs_mid, two_send)
    for g in range(2):
        settle(sums_in.at[g], sum_send.at[g])

    up = sum(LIFT)
    down = 2 * nc - up

    @pl.when(z == 0)
    def _():
        for i, count in enumerate((2 * nc, up)):
            settle(sums_far.at[0], far_send.at[i])
            settle(blocks(count), k_send.at[i])
            settle(blocks(count), v_send.at[i])

    @pl.when(z == 1)
    def _():
        settle(sums_far.at[0], far_send.at[0])
        settle(blocks(up), k_send.at[1])
        settle(blocks(up), v_send.at[1])
        for i in range(2):
            settle(lse_msg, l_send.at[i])
            settle(blocks(down), o_send.at[i])

    @pl.when(z == 2)
    def _():
        for i in range(2):
            settle(sums_far.at[0], far_send.at[i])
        settle(lse_msg, l_send.at[0])
        settle(blocks(LIFT[0] + nc), o_send.at[0])
        settle(blocks(down), q_send.at[0])
        settle(blocks(nc - LIFT[0]), k_send.at[2])
        settle(blocks(nc - LIFT[0]), v_send.at[2])

    @pl.when(z == 3)
    def _():
        for i, count in enumerate((LIFT[0] + nc, down)):
            settle(sums_far.at[0], far_send.at[i])
            settle(blocks(count), q_send.at[i])

    _t.__exit__(None, None, None)


def fused(ns, nt, tokens, w_query, w_key, w_value, w_out, gain_query, gain_key):
    tok, seqs, depth = tokens.shape
    local = w_query.shape[1]
    nc = local // COLS
    oc = 1024
    no = depth // oc
    rows = tok * seqs
    width = HEADS * HEAD_DIM
    vm = pltpu.VMEM
    dma = pltpu.SemaphoreType.DMA
    scratch = [
        vm((local,), F32), vm((local,), F32),
        vm((RING, depth, COLS), BF16), vm((no, local, oc), BF16),
        vm((tok, seqs, depth), BF16), vm((rows, depth), BF16), vm((rows, depth), BF16),
        vm((rows, HEAD_DIM), F32), vm((rows, HEAD_DIM), F32), vm((2, nc, 1, COLS), F32), vm((2, rows, HEAD_DIM), F32),
        vm((2, 8, rows), F32), vm((2, nt - 1, 8, rows), F32), vm((3, nt, 8, rows), F32),
        vm((3, rows, 2 * rows), F32), vm((2, 8, 2 * rows), F32),
        vm((2, nc, seqs, 3 * tok, COLS), BF16), vm((nc, seqs, 3 * tok, COLS), BF16),
        vm((nc, seqs, tok, COLS), F32), vm((seqs, tok, HEAD_DIM), F32),
        vm((2, nc, seqs, tok, COLS), BF16), vm((seqs, 2, tok, HEAD_DIM), F32), vm((seqs, 16, rows), F32),
        vm((2, nc, seqs, tok, COLS), BF16), vm((2, seqs, 16, rows), F32), vm((3, tok, HEAD_DIM), F32),
        vm((rows, local), BF16), vm((no, seqs, 2, 2, 2, tok // nt, oc // 2), BF16),
        vm((no, seqs, 2, 2, tok // nt, oc // 2), BF16), vm((no, seqs, 2, tok // nt, oc // 2), BF16), vm((no, seqs, 2, tok // nt, oc // 2), BF16),
        dma, dma((2,)), dma((RING,)), dma((no,)), dma((2,)), dma((2,)), dma((2,)), dma((3,)), dma((3,)), dma((3,)), dma((2, nc)),
        dma((2,)), dma((2, nc)), dma((2,)), dma((2, nc)), dma((2,)), dma((2,)), dma, dma((2, no)), dma, dma((2, no)),
    ]
    in_vmem = pl.BlockSpec(memory_space=pltpu.VMEM)
    in_hbm = pl.BlockSpec(memory_space=pltpu.HBM)
    return pl.pallas_call(
        functools.partial(block_kernel, ns, nt, tok, width),
        out_shape=pltpu.VMEM((tok // nt, seqs, depth), BF16),
        in_specs=[in_hbm] * 7,
        out_specs=in_vmem,
        scratch_shapes=scratch,
        compiler_params=pltpu.CompilerParams(collective_id=0, has_side_effects=True, vmem_limit_bytes=58 * 1024 * 1024),
    )(tokens, gain_query, gain_key, w_query, w_key, w_value, w_out)


def rotary(field, positions):
    half = HEAD_DIM // 2
    shaped = field.reshape(field.shape[0], -1, HEAD_DIM)
    freqs = jnp.exp(-jnp.log(500000.0) * jnp.arange(half, dtype=jnp.float32) * 2.0 / HEAD_DIM)
    angle = positions.astype(jnp.float32)[:, None] * freqs[None, :]
    cosine = jnp.cos(angle)[:, None, :]
    sine = jnp.sin(angle)[:, None, :]
    first = shaped[..., :half]
    second = shaped[..., half:]
    turned = jnp.concatenate(
        [first * cosine - second * sine, second * cosine + first * sine], axis=-1
    )
    return turned.reshape(field.shape[0], -1)


def local(tokens, w_query, w_key, w_value, w_out, gain_query, gain_key):
    tok_rows = tokens.shape[0]
    seq_count = tokens.shape[1]
    local_width = w_query.shape[1]
    local_heads = local_width // HEAD_DIM
    width = HEADS * HEAD_DIM
    flat = tokens.reshape(tok_rows * seq_count, tokens.shape[2])
    query = jnp.dot(flat, w_query, preferred_element_type=jnp.float32)
    key_raw = jnp.dot(flat, w_key, preferred_element_type=jnp.float32)
    sum_query, sum_key = lax.psum(
        (jnp.sum(query * query, axis=1), jnp.sum(key_raw * key_raw, axis=1)), "tensor"
    )
    value = jnp.dot(flat, w_value, preferred_element_type=jnp.float32).astype(jnp.bfloat16)
    scale_q = lax.rsqrt(sum_query / width + 1e-06)
    scale_k = lax.rsqrt(sum_key / width + 1e-06)
    my_block = lax.axis_index("seq")
    positions = my_block * tok_rows + jnp.arange(tok_rows, dtype=jnp.int32)
    row_positions = (positions[:, None] + jnp.zeros((1, seq_count), jnp.int32)).reshape(-1)
    q_normed = rotary(query * scale_q[:, None] * gain_query[None, :], row_positions).astype(
        jnp.bfloat16
    )
    k_normed = rotary(key_raw * scale_k[:, None] * gain_key[None, :], row_positions).astype(
        jnp.bfloat16
    )
    q_heads = q_normed.reshape(tok_rows, seq_count, local_heads, HEAD_DIM)
    k_local = k_normed.reshape(tok_rows, seq_count, local_width)
    v_local = value.reshape(tok_rows, seq_count, local_width)
    factor = HEAD_DIM ** (-0.5)
    piece = (
        lax.all_gather(k_local, "seq", axis=0, tiled=True),
        lax.all_gather(v_local, "seq", axis=0, tiled=True),
    )
    key_pos = jnp.arange(piece[0].shape[0], dtype=jnp.int32)
    key_block = piece[0]
    count = key_block.shape[0]
    key_heads = key_block.reshape(count, seq_count, local_heads, HEAD_DIM)
    value_heads = piece[1].reshape(count, seq_count, local_heads, HEAD_DIM)
    scores = (
        jnp.einsum("qshd,kshd->shqk", q_heads, key_heads, preferred_element_type=jnp.float32)
        * factor
    )
    allowed = (key_pos[None, None, None, :] <= positions[None, None, :, None]) & (
        key_pos[None, None, None, :] >= 0
    )
    old_max = jnp.full((seq_count, local_heads, tok_rows), -1e30, jnp.float32)
    new_max = jnp.maximum(old_max, jnp.max(jnp.where(allowed, scores, -1e30), axis=3))
    expo = jnp.where(allowed, jnp.exp(scores - new_max[..., None]), 0.0)
    new_total = jnp.sum(expo, axis=3)
    added = jnp.einsum(
        "shqk,kshd->shqd",
        expo.astype(jnp.bfloat16),
        value_heads,
        preferred_element_type=jnp.float32,
    )
    final_state = (new_max, new_total, added)
    final_max, final_total, final_acc = final_state
    mixed = (final_acc / final_total[..., None]).astype(jnp.bfloat16)
    mixed = jnp.transpose(mixed, (2, 0, 1, 3)).reshape(tok_rows, seq_count, local_width)
    return lax.psum_scatter(
        jnp.dot(mixed, w_out, preferred_element_type=jnp.float32).astype(jnp.bfloat16),
        "tensor",
        scatter_dimension=0,
        tiled=True,
    )


def solution(mesh):
    ns, nt = mesh.shape["seq"], mesh.shape["tensor"]
    step = functools.partial(fused, ns, nt) if ns == 4 and nt == 4 else local
    return jax.shard_map(
        step,
        mesh=mesh,
        in_specs=(
            P("seq", "dp", None),
            P(None, "tensor"),
            P(None, "tensor"),
            P(None, "tensor"),
            P("tensor", None),
            P("tensor"),
            P("tensor"),
        ),
        out_specs=P(("seq", "tensor"), "dp", None),
        check_vma=False,
    )
```
